128 devices in a mesh: dp: 2 (over y_lo), section: 4 (over z), mp: 16 (over x, y_hi, core).
Axes of the slice: x: 4, y: 4 (y_hi: 2, y_lo: 2; y = y_hi * 2 + y_lo), z: 4, core: 2. Of those that a mesh axis runs over, the one named last changes fastest.
Arguments:
- token_ids: int32 [32, 32], P('dp'), may hold values from 0 to 65535
- members: int32 [32], replicated, may hold values from 0 to 31, each once
- owners: int32 [4], replicated, may hold values from 0 to 3, each once
- embed_table: bfloat16 [4096, 65536], P('mp', 'section'), may hold values from -6 to 6
- norm_gain: float32 [4, 4096], P('section'), may hold values from 0.5 to 2
- gate_weight: bfloat16 [4, 4096, 10240], P('section', None, 'mp'), may hold values from -0.09375 to 0.09375
- up_weight: bfloat16 [4, 4096, 10240], P('section', None, 'mp'), may hold values from -0.09375 to 0.09375
- down_weight: bfloat16 [4, 4096, 10240], P('section', None, 'mp'), may hold values from -0.078125 to 0.078125
- final_gain: float32 [4096], replicated, may hold values from 0.5 to 2
- head_weight: bfloat16 [4096, 4096], P(None, 'mp'), may hold values from -0.0014648438 to 0.0014648438
Outputs:
- wins: float32 [4, 8, 8], P('dp', 'section')
The draws below stay inside these ranges and needn't reach their ends.
Inputs may be any that keep to these rules, and one draw needn't show every extreme that they name: Prompt p's responses are members[8 * p] to members[8 * p + 7]; each response belongs to one prompt. `owners`: each slot holds one prompt.
All inputs are finite; a program needn't handle non-finite values.
Results may differ from the reference program's by a relative error of at most 0.028.
Values may be sent and summed in bfloat16 or wider, within the bound.
No kernel may reach another device: no remote copies, remote signals or barrier semaphores. Data moves between devices by JAX's collectives and lax.ppermute only.
A program may use at most 128 MiB of HBM per device.

```python
import math
import jax
import jax.numpy as jnp
from jax import lax

D = 4096
FF = 10240
VOCAB = 65536
LENGTH = 32
GROUP = 8
LAYERS = 4
RESPONSES = 32
PROMPTS = 4
N_MP = 16


def place_ends(drawn, own_key, smallest, largest):
    longest = drawn.shape.index(max(drawn.shape))
    spots = []
    for shift in (0, 1):
        where = [jax.random.randint(jax.random.fold_in(own_key, axis), (), 0, length) for axis, length in enumerate(drawn.shape)]
        where[longest] = (where[longest] + shift) % drawn.shape[longest]
        spots.append(tuple(where))
    return drawn.at[spots[0]].set(smallest).at[spots[1]].set(largest)


def raised(drawn, key, source, target, blocks, factor):
    def block_of(position):
        return (jnp.arange(drawn.shape[position]) // (drawn.shape[position] // blocks)).reshape((-1,) + (1,) * (drawn.ndim - 1 - position))

    first = jax.random.permutation(key, blocks)[block_of(target)]
    second = (block_of(target) + blocks // 2) % blocks
    return jnp.where((block_of(source) == first) | (block_of(source) == second), factor * drawn, drawn)


def level_of(own_key, extent, split, smallest, top_value):
    def one(dim, shards_of):
        steps = jax.random.uniform(jax.random.fold_in(jax.random.fold_in(own_key, 6), dim), (shards_of,), jnp.float32, smallest / len(split), top_value / len(split))
        return jnp.repeat(jnp.exp(steps), extent[dim] // shards_of).reshape((-1,) + (1,) * (len(extent) - dim - 1))

    loudness = one(*split[0])
    for cut in split[1:]:
        loudness = loudness * one(*cut)
    return loudness


def noise(key, extent, scale, limit, split=(), dtype=jnp.bfloat16):
    level = level_of(key, extent, split, -0.22, 0.18) if split else 1.0
    result = jax.random.normal(key, extent, jnp.float32) * scale * level
    return jnp.minimum(jnp.maximum(result, -limit), limit).astype(dtype)


def heavy_noise(rng, dims, scale, bound, split, heavy, dtype=jnp.bfloat16):
    drawn = scale * jax.random.normal(rng, dims, jnp.float32)
    if split:
        drawn = drawn * level_of(rng, dims, split, -0.22, 0.18)
    return jnp.clip(raised(drawn, jax.random.fold_in(rng, 3), *heavy), -bound, bound).astype(dtype)


def setup_inputs(seed: int = 0) -> dict:
    key_list = jax.random.split(jax.random.key(seed), 11)
    token_ids = place_ends(jax.random.randint(key_list[0], (RESPONSES, LENGTH), 0, VOCAB), jax.random.fold_in(key_list[0], 1), 0, VOCAB - 1).astype(jnp.int32)
    members = jax.random.permutation(key_list[1], RESPONSES).astype(jnp.int32)
    owners = jax.random.permutation(key_list[2], PROMPTS).astype(jnp.int32)
    embed_table = noise(key_list[3], (D, VOCAB), 1.0, 6.0, ((0, 16), (1, 4)))
    norm_gain = jnp.clip(jnp.exp(math.log(2.0) - 1.3862944 * jax.random.uniform(key_list[4], (LAYERS, D), jnp.float32) ** level_of(key_list[4], (LAYERS, D), ((0, 4),), -0.2, 0.2)), 0.5, 2.0)
    gate_weight = noise(key_list[5], (LAYERS, D, FF), D ** -0.5, 0.09375, ((0, 4), (2, 16)))
    up_weight = noise(key_list[6], (LAYERS, D, FF), D ** -0.5, 0.09375, ((0, 4), (2, 16)))
    down_weight = heavy_noise(key_list[7], (LAYERS, D, FF), FF ** -0.5, 0.078125, ((0, 4), (2, 16)), (2, 1, 16, 2.0))
    final_gain = jnp.clip(jnp.exp(jax.random.uniform(key_list[8], (D,), jnp.float32, math.log(0.5), math.log(2.0))), 0.5, 2.0)
    head_weight = noise(key_list[9], (D, D), (D * D) ** -0.5, 0.0014648438, ((1, 16),))
    return dict(token_ids=token_ids, members=members, owners=owners, embed_table=embed_table, norm_gain=norm_gain, gate_weight=gate_weight, up_weight=up_weight, down_weight=down_weight, final_gain=final_gain, head_weight=head_weight)


norm_eps = 1e-05
final_eps = 1e-06

def contract_rows(weights, acts):
    return lax.dot_general(weights, acts, (((0,), (0,)), ((), ())), preferred_element_type=jnp.float32)

def reference(token_ids, members, owners, embed_table, norm_gain, gate_weight, up_weight, down_weight, final_gain, head_weight):
    state = jnp.take(embed_table, token_ids.reshape(-1), axis=1)
    block = FF // N_MP
    for layer in range(LAYERS):
        wide = state.astype(jnp.float32)
        scaled = (wide * norm_gain[layer][:, None]).astype(jnp.bfloat16)
        inverse = lax.rsqrt(lax.optimization_barrier(jnp.mean(wide * wide, axis=0, keepdims=True)) + norm_eps)
        gate = contract_rows(gate_weight[layer], scaled) * inverse
        upper = contract_rows(up_weight[layer], scaled) * inverse
        hidden = (jax.nn.silu(gate) * upper).astype(jnp.bfloat16)
        w_down = down_weight[layer]

        def add_block(index, total):
            start = (index * block).astype(jnp.int32)
            part = jnp.dot(lax.dynamic_slice_in_dim(w_down, start, block, 1), lax.dynamic_slice_in_dim(hidden, start, block, 0), preferred_element_type=jnp.float32)
            rounded = lax.optimization_barrier(part.astype(jnp.bfloat16))
            return total + rounded.astype(jnp.float32)
        total = lax.fori_loop(jnp.int32(0), jnp.int32(N_MP), add_block, jnp.zeros(wide.shape, jnp.float32))
        state = (wide + total).astype(jnp.bfloat16)
    pooled = lax.optimization_barrier(jnp.mean(state.astype(jnp.float32).reshape(D, RESPONSES, LENGTH), axis=2))
    factor = lax.rsqrt(lax.optimization_barrier(jnp.mean(pooled * pooled, axis=0, keepdims=True)) + final_eps)
    normed = (pooled * factor * final_gain[:, None]).astype(jnp.bfloat16)
    projected = contract_rows(head_weight, normed)
    scores = lax.dot_general(projected, normed.astype(jnp.float32), (((0,), (0,)), ((), ())), precision=lax.Precision.HIGHEST, preferred_element_type=jnp.float32)
    preference = jax.nn.sigmoid(scores - scores.T)
    groups = members.reshape(PROMPTS, GROUP)
    tiles = preference[groups[:, :, None], groups[:, None, :]]
    return jnp.zeros((PROMPTS, GROUP, GROUP), jnp.float32).at[owners].set(tiles)
```

```python
import functools

import jax
import jax.numpy as jnp
from jax import lax
from jax.experimental import pallas as pl
from jax.experimental.pallas import tpu as pltpu
from jax.sharding import PartitionSpec as P

GROUP = 8
BLOCKS = 2
AXES = ("dp", "section", "mp")

norm_eps = 1e-05
final_eps = 1e-06
bf16 = jnp.bfloat16
f32 = jnp.float32


def moved(value, target):
    pairs = []
    for dp in range(2):
        for z in range(4):
            for x in range(4):
                for y in range(2):
                    for c in range(2):
                        to = target(dp, z, x, y, c)
                        if to is not None:
                            d, s, a, b, e = to
                            pairs.append(
                                (dp * 64 + z * 16 + x * 4 + y * 2 + c, d * 64 + s * 16 + a * 4 + b * 2 + e)
                            )
    return lax.ppermute(value, AXES, pairs)


def along_x(value, shift):
    return moved(value, lambda d, z, x, y, c: (d, z, (x + shift) % 4, y, c))


def other_core(value):
    return moved(value, lambda d, z, x, y, c: (d, z, x, y, 1 - c))


def other_y(value):
    return moved(value, lambda d, z, x, y, c: (d, z, x, 1 - y, c))


def to_first(value, source):
    return moved(value, lambda d, z, x, y, c: (d, 0, x, y, c) if z == source else None)


def onward(value, flip):
    return moved(value, lambda d, z, x, y, c: (d, z + 1, x, y ^ flip, c) if z < 3 else None)


def nt_dot(a, b):
    return lax.dot_general(a, b, (((1,), (1,)), ((), ())), preferred_element_type=f32)


def embed_kernel(ids_ref, table_ref, out_ref, acc_ref):
    step = pl.program_id(0)
    width = table_ref.shape[1]

    @pl.when(step == 0)
    def _():
        acc_ref[...] = jnp.zeros_like(acc_ref)

    here = ids_ref[...] - step * width
    hot = lax.broadcasted_iota(jnp.int32, (ids_ref.shape[0], width), 1) == here
    acc_ref[...] += nt_dot(hot.astype(f32).astype(bf16), table_ref[...])

    @pl.when(step == pl.num_programs(0) - 1)
    def _():
        out_ref[...] = acc_ref[...].astype(bf16)


def embed_part(ids, table):
    count, rows, vocab = ids.shape[0], table.shape[0], table.shape[1]
    width = 2048
    return pl.pallas_call(
        embed_kernel,
        grid=(vocab // width,),
        in_specs=[
            pl.BlockSpec((count, 1), lambda i: (0, 0)),
            pl.BlockSpec((rows, width), lambda i: (0, i)),
        ],
        out_specs=pl.BlockSpec((count, rows), lambda i: (0, 0)),
        out_shape=jax.ShapeDtypeStruct((count, rows), bf16),
        scratch_shapes=[pltpu.VMEM((count, rows), f32)],
        name="embed",
    )(ids, table)


def prepare(x, c, chunks, gain_ref, scaled_ref):
    squares = None
    for shift in range(4):
        base = lax.rem(x + 4 - shift, 4) * 1024
        for ref, core in ((chunks[shift], c), (chunks[4 + shift], 1 - c)):
            for y in range(2):
                block = ref[:, y * 256 : (y + 1) * 256].astype(f32)
                off = pl.multiple_of(base + y * 512 + core * 256, 256)
                scaled_ref[:, pl.ds(off, 256)] = (block * gain_ref[:, pl.ds(off, 256)]).astype(bf16)
                part = block[:, :128] * block[:, :128] + block[:, 128:] * block[:, 128:]
                squares = part if squares is None else squares + part
    return lax.rsqrt(jnp.sum(squares, axis=1, keepdims=True) / 4096 + norm_eps)


def hidden_units(scaled_ref, vg, vu, waits, inverse):
    gate = up = None
    for k in range(4):
        waits[2 * k].wait()
        part = scaled_ref[:, k * 1024 : (k + 1) * 1024]
        now = jnp.dot(part, vg[k * 1024 : (k + 1) * 1024, :], preferred_element_type=f32)
        gate = now if gate is None else gate + now
        waits[2 * k + 1].wait()
        now = jnp.dot(part, vu[k * 1024 : (k + 1) * 1024, :], preferred_element_type=f32)
        up = now if up is None else up + now
    gate = gate * inverse
    return gate / (1.0 + jnp.exp(-gate)) * (up * inverse)


def mean_tokens(value):
    rows, cols = value.shape
    return jnp.sum(value.reshape(rows // 32, 32, cols), axis=1) * (1.0 / 32)


def weight_copies(refs, scratch, sems, down_rows):
    wg, wu, wd = refs
    vg, vu, vd = scratch
    copies = []
    for k in range(4):
        rows = pl.ds(k * 1024, 1024)
        copies.append(pltpu.make_async_copy(wg.at[0, rows, :], vg.at[rows, :], sems.at[2 * k]))
        copies.append(pltpu.make_async_copy(wu.at[0, rows, :], vu.at[rows, :], sems.at[2 * k + 1]))
    for k in range(4):
        rows = pl.ds(down_rows[k], 1024)
        place = pl.ds(k * 1024, 1024)
        copies.append(pltpu.make_async_copy(wd.at[0, rows, :], vd.at[place, :], sems.at[8 + k]))
    for copy in copies:
        copy.start()
    return copies


ORDER = (2, 1, 3, 0)


def mlp_kernel(place, *refs):
    chunks, (gain, wg, wu, wd), (send, keep, pooled) = refs[:8], refs[8:12], refs[12:15]
    vg, vu, vd, scaled, sems = refs[15:]
    x, c = place[0], place[1]
    down_rows = [pl.multiple_of(lax.rem(x + s, 4) * 1024, 1024) for s in ORDER]
    copies = weight_copies((wg, wu, wd), (vg, vu, vd), sems, down_rows)
    inverse = prepare(x, c, chunks, gain, scaled)
    hidden = hidden_units(scaled, vg, vu, copies, inverse)
    pooled[...] = mean_tokens(hidden)
    rounded = hidden.astype(bf16)
    first = c == 0
    for k, s in enumerate(ORDER):
        copies[8 + k].wait()
        term = nt_dot(rounded, vd[k * 1024 : (k + 1) * 1024, :])
        for y in range(2):
            a = term[:, y * 512 : y * 512 + 256]
            b = term[:, y * 512 + 256 : y * 512 + 512]
            cols = slice(y * 256, (y + 1) * 256)
            keep[s, :, cols] = jnp.where(first, a, b).astype(bf16)
            send[s, :, cols] = jnp.where(first, b, a).astype(bf16)


def last_kernel(place, *refs):
    chunks, (gain, before, wg, wu, wd), (out,) = refs[:8], refs[8:13], refs[13:14]
    vg, vu, vd, scaled, sems = refs[14:]
    x, c = place[0], place[1]
    copies = weight_copies((wg, wu, wd), (vg, vu, vd), sems, [0, 1024, 2048, 3072])
    inverse = prepare(x, c, chunks, gain, scaled)
    hidden = hidden_units(scaled, vg, vu, copies, inverse)
    both = jnp.concatenate([before[...], mean_tokens(hidden)], axis=0)
    high = both.astype(bf16)
    low = (both - high.astype(f32)).astype(bf16)
    count = both.shape[0]
    stacked = jnp.concatenate([high, low], axis=0)
    for k in range(4):
        copies[8 + k].wait()
        term = nt_dot(stacked, vd[k * 1024 : (k + 1) * 1024, :])
        term = term[:count] + term[count:]
        for m in range(4):
            out[4 * k + m] = term[:, m * 256 : (m + 1) * 256]


def call_mlp(place, mine, theirs, gain, weights, before=None):
    tokens = mine[0].shape[0]
    width = 640
    vmem = pl.BlockSpec(memory_space=pltpu.VMEM)
    hbm = pl.BlockSpec(memory_space=pl.ANY)
    smem = pl.BlockSpec(memory_space=pltpu.SMEM)
    responses = tokens // 32
    if before is None:
        kernel, extra, name = mlp_kernel, [], "mlp"
        out_shape = [
            jax.ShapeDtypeStruct((4, tokens, 512), bf16),
            jax.ShapeDtypeStruct((4, tokens, 512), bf16),
            jax.ShapeDtypeStruct((responses, width), f32),
        ]
        out_specs = [vmem] * 3
    else:
        kernel, extra, name = last_kernel, [before], "last_mlp"
        out_shape = jax.ShapeDtypeStruct((16, before.shape[0] + responses, 256), f32)
        out_specs = vmem
    return pl.pallas_call(
        kernel,
        in_specs=[smem] + [vmem] * (9 + len(extra)) + [hbm] * 3,
        out_specs=out_specs,
        out_shape=out_shape,
        scratch_shapes=[
            pltpu.VMEM((4096, width), bf16),
            pltpu.VMEM((4096, width), bf16),
            pltpu.VMEM((4096, width), bf16),
            pltpu.VMEM((tokens, 4096), bf16),
            pltpu.SemaphoreType.DMA((12,)),
        ],
        compiler_params=pltpu.CompilerParams(vmem_limit_bytes=56 * 1024 * 1024),
        name=name,
    )(place, *mine, *theirs, gain, *extra, *weights)


def head_kernel(place, chosen_ref, all_ref, gain_ref, head_ref, out_ref):
    total = squares = None
    for m in range(16):
        cols = slice(m * 256, (m + 1) * 256)
        v = jnp.concatenate([all_ref[0, m], all_ref[1, m]], axis=0)
        now = jnp.dot(v, head_ref[cols, :], preferred_element_type=f32)
        total = now if total is None else total + now
        plain = v.astype(f32) / gain_ref[:, cols]
        plain = plain * plain
        plain = plain[:, :128] + plain[:, 128:]
        squares = plain if squares is None else squares + plain
    factor = lax.rsqrt(jnp.sum(squares, axis=1, keepdims=True) / 4096 + final_eps)
    here = place[0]
    mine = jnp.concatenate([all_ref[0, here], all_ref[1, here]], axis=0).astype(f32) * factor
    scores = lax.dot_general(
        total * factor, mine, (((1,), (1,)), ((), ())),
        precision=lax.Precision.HIGHEST, preferred_element_type=f32,
    )
    skew = scores - scores.T
    chosen = chosen_ref[...]
    count = skew.shape[0]
    hot = (lax.broadcasted_iota(jnp.int32, (chosen.shape[0], count), 1) == chosen).astype(f32)
    rows = jnp.dot(hot, skew, precision=lax.Precision.HIGHEST, preferred_element_type=f32)
    out_ref[...] = lax.dot_general(
        rows, hot, (((1,), (1,)), ((), ())),
        precision=lax.Precision.HIGHEST, preferred_element_type=f32,
    )


def head_part(place, chosen, everyone, gain, head):
    vmem = pl.BlockSpec(memory_space=pltpu.VMEM)
    return pl.pallas_call(
        head_kernel,
        in_specs=[pl.BlockSpec(memory_space=pltpu.SMEM)] + [vmem] * 4,
        out_specs=vmem,
        out_shape=jax.ShapeDtypeStruct((chosen.shape[0], chosen.shape[0]), f32),
        name="head",
    )(place, chosen, everyone, gain, head)


def per_device(
    token_ids, members, owners, embed_table, norm_gain, gate_weight, up_weight, down_weight,
    final_gain, head_weight,
):
    section = lax.axis_index("section")
    mp = lax.axis_index("mp")
    dp = lax.axis_index("dp")
    x, y, c = mp // 4, (mp // 2) % 2, mp % 2
    place = jnp.stack([x, c]).astype(jnp.int32)
    weights = (gate_weight, up_weight, down_weight)
    flat = token_ids.reshape(-1, 1) - section * embed_table.shape[1]
    block = flat.shape[0] // BLOCKS

    def fresh(index):
        part = embed_part(flat[index * block : (index + 1) * block], embed_table)
        pieces = [to_first(part, z) for z in (1, 3, 2)]
        own = part + pieces[0] + pieces[1] + pieces[2]
        peer = other_y(own)
        return jnp.where(
            y == 0, jnp.concatenate([own, peer], axis=1), jnp.concatenate([peer, own], axis=1)
        )

    blocks = [fresh(i) for i in range(BLOCKS)]
    state = None
    sums_state, sums_hidden = [], []
    ticks = BLOCKS + 3
    for tick in range(ticks):
        if tick < BLOCKS:
            state = blocks[tick] if tick == 0 else jnp.where(section == 0, blocks[tick], state)
        if tick >= 3:
            sums_state.append(mean_tokens(state.astype(f32)))
        mine = [state] + [along_x(state, s) for s in (1, 2, 3)]
        theirs = [other_core(m) for m in mine]
        if tick == ticks - 1:
            before = jnp.concatenate(sums_hidden, axis=0)
            terms = call_mlp(place, mine, theirs, norm_gain, weights, before)
            break
        send, keep, pooled = call_mlp(place, mine, theirs, norm_gain, weights)
        if tick >= 3:
            sums_hidden.append(pooled)
        halves = [
            (keep[s].astype(f32) + other_core(send[s]).astype(f32)) for s in range(4)
        ]
        arrived = [along_x(halves[s].astype(bf16), s) for s in (2, 1, 3)]
        total = halves[0] + jnp.where(y == 0, state.astype(f32), 0.0)
        for a in arrived:
            total = total + a.astype(f32)
        total = total.astype(bf16)
        state = (onward(total, 0).astype(f32) + onward(total, 1).astype(f32)).astype(bf16)

    pieces = lax.all_to_all(terms, "mp", 0, 0, tiled=True)
    base = jnp.concatenate(sums_state, axis=0)
    pooled = jnp.sum(pieces, axis=0) + jnp.where(y == 0, base[:, :256], base[:, 256:])
    gain_here = lax.dynamic_slice_in_dim(final_gain, mp * 256, 256)
    value = (pooled * gain_here[None, :]).astype(bf16)
    everyone = lax.all_to_all(
        jnp.broadcast_to(value, (32, *value.shape)), ("dp", "mp"), 0, 0, tiled=True
    ).reshape(2, 16, *value.shape)

    prompts = owners.shape[0]
    here = prompts // 2
    slots = dp * here + jnp.arange(here, dtype=jnp.int32)
    match = (owners[None, :] == slots[:, None]).astype(jnp.int32)
    hit = match[:, :, None] * members.reshape(prompts, GROUP)[None]
    chosen = jnp.sum(hit, axis=1).reshape(here * GROUP, 1)
    tile = head_part(
        jnp.reshape(mp, (1,)).astype(jnp.int32), chosen, everyone, final_gain[None], head_weight
    )
    rows = GROUP // 4
    parts = jnp.stack([tile[p * GROUP : (p + 1) * GROUP, p * GROUP : (p + 1) * GROUP] for p in range(here)])
    parts = jnp.swapaxes(parts.reshape(here, 4, rows, GROUP), 0, 1).reshape(4, 1, 1, -1)
    parts = jnp.broadcast_to(parts, (4, 16, 1, parts.shape[-1])).reshape(64, 1, -1)
    got = lax.all_to_all(parts, ("section", "mp"), 0, 0, tiled=True)
    skew = jnp.sum(got[48:], axis=(0, 1))
    return jax.nn.sigmoid(skew).reshape(here, rows, GROUP)


def solution(mesh):
    placed = (
        P("dp", None),
        P(),
        P(),
        P("mp", "section"),
        P("section", None),
        P("section", None, "mp"),
        P("section", None, "mp"),
        P("section", None, "mp"),
        P(),
        P(None, "mp"),
    )
    return jax.shard_map(
        per_device, mesh=mesh, in_specs=placed, out_specs=P("dp", "section", None), check_vma=False
    )
```

```python
import functools

import jax
import jax.numpy as jnp
from jax import lax
from jax.experimental import pallas as pl
from jax.experimental.pallas import tpu as pltpu
from jax.sharding import PartitionSpec as P

GROUP = 8
BLOCKS = 4
STREAMS = 2
AXES = ("dp", "section", "mp")

norm_eps = 1e-05
final_eps = 1e-06
bf16 = jnp.bfloat16
f32 = jnp.float32


def moved(value, target):
    pairs = []
    for dp in range(2):
        for z in range(4):
            for x in range(4):
                for y in range(2):
                    for c in range(2):
                        to = target(dp, z, x, y, c)
                        if to is not None:
                            d, s, a, b, e = to
                            pairs.append(
                                (dp * 64 + z * 16 + x * 4 + y * 2 + c, d * 64 + s * 16 + a * 4 + b * 2 + e)
                            )
    return lax.ppermute(value, AXES, pairs)


def along_x(value, shift):
    return moved(value, lambda d, z, x, y, c: (d, z, (x + shift) % 4, y, c))


def other_core(value):
    return moved(value, lambda d, z, x, y, c: (d, z, x, y, 1 - c))


def other_y(value):
    return moved(value, lambda d, z, x, y, c: (d, z, x, 1 - y, c))


def to_first(value, source):
    return moved(value, lambda d, z, x, y, c: (d, 0, x, y, c) if z == source else None)


def onward(value, flip):
    return moved(value, lambda d, z, x, y, c: (d, z + 1, x, y ^ flip, c) if z < 3 else None)


def nt_dot(a, b):
    return lax.dot_general(a, b, (((1,), (1,)), ((), ())), preferred_element_type=f32)


def embed_kernel(ids_ref, table_ref, out_ref, acc_ref):
    step = pl.program_id(0)
    width = table_ref.shape[1]

    @pl.when(step == 0)
    def _():
        acc_ref[...] = jnp.zeros_like(acc_ref)

    here = ids_ref[...] - step * width
    hot = lax.broadcasted_iota(jnp.int32, (ids_ref.shape[0], width), 1) == here
    acc_ref[...] += nt_dot(hot.astype(f32).astype(bf16), table_ref[...])

    @pl.when(step == pl.num_programs(0) - 1)
    def _():
        out_ref[...] = acc_ref[...].astype(bf16)


def embed_part(ids, table):
    count, rows, vocab = ids.shape[0], table.shape[0], table.shape[1]
    width = 2048
    return pl.pallas_call(
        embed_kernel,
        grid=(vocab // width,),
        in_specs=[
            pl.BlockSpec((count, 1), lambda i: (0, 0)),
            pl.BlockSpec((rows, width), lambda i: (0, i)),
        ],
        out_specs=pl.BlockSpec((count, rows), lambda i: (0, 0)),
        out_shape=jax.ShapeDtypeStruct((count, rows), bf16),
        scratch_shapes=[pltpu.VMEM((count, rows), f32)],
        name="embed",
    )(ids, table)


def prepare(x, c, chunks, gain_ref, scaled_ref):
    squares = None
    for shift in range(4):
        base = lax.rem(x + 4 - shift, 4) * 1024
        for ref, core in ((chunks[shift], c), (chunks[4 + shift], 1 - c)):
            for y in range(2):
                block = ref[:, y * 256 : (y + 1) * 256].astype(f32)
                off = pl.multiple_of(base + y * 512 + core * 256, 256)
                scaled_ref[:, pl.ds(off, 256)] = (block * gain_ref[:, pl.ds(off, 256)]).astype(bf16)
                part = block[:, :128] * block[:, :128] + block[:, 128:] * block[:, 128:]
                squares = part if squares is None else squares + part
    return lax.rsqrt(jnp.sum(squares, axis=1, keepdims=True) / 4096 + norm_eps)


def hidden_units(scaled, wg, wu, inverse):
    gate = jnp.dot(scaled, wg, preferred_element_type=f32) * inverse
    up = jnp.dot(scaled, wu, preferred_element_type=f32)
    return gate / (1.0 + jnp.exp(-gate)) * (up * inverse)


def mean_tokens(value):
    rows, cols = value.shape
    return jnp.sum(value.reshape(rows // 32, 32, cols), axis=1) * (1.0 / 32)


def mlp_kernel(place, *refs):
    chunks, (gain, wg, wu, wd), (send, keep, pooled, scaled) = refs[:8], refs[8:12], refs[12:]
    x, c = place[0], place[1]
    inverse = prepare(x, c, chunks, gain, scaled)
    hidden = hidden_units(scaled[...], wg[0], wu[0], inverse)
    pooled[...] = mean_tokens(hidden)
    rounded = hidden.astype(bf16)
    first = c == 0

    def one(s, carry):
        rows = pl.multiple_of(lax.rem(x + s, 4) * 1024, 1024)
        term = nt_dot(rounded, wd[0, pl.ds(rows, 1024), :])
        for y in range(2):
            a = term[:, y * 512 : y * 512 + 256]
            b = term[:, y * 512 + 256 : y * 512 + 512]
            cols = slice(y * 256, (y + 1) * 256)
            keep[s, :, cols] = jnp.where(first, a, b).astype(bf16)
            send[s, :, cols] = jnp.where(first, b, a).astype(bf16)
        return carry

    lax.fori_loop(0, 4, one, 0)


def last_kernel(count, place, *refs):
    chunks, (gain, wg, wu, wd) = refs[:8], refs[8:12]
    before, out, scaled = refs[12 : 12 + count], refs[-2], refs[-1]
    x, c = place[0], place[1]
    inverse = prepare(x, c, chunks, gain, scaled)
    hidden = hidden_units(scaled[...], wg[0], wu[0], inverse)
    every = jnp.concatenate([ref[...] for ref in before] + [mean_tokens(hidden)], axis=0)
    high = every.astype(bf16)
    low = (every - high.astype(f32)).astype(bf16)
    rows = every.shape[0]
    stacked = jnp.concatenate([high, low], axis=0)

    def one(m, carry):
        term = nt_dot(stacked, wd[0, pl.ds(pl.multiple_of(m * 256, 256), 256), :])
        out[m] = term[:rows] + term[rows:]
        return carry

    lax.fori_loop(0, 16, one, 0)


def halves_kernel(keep, got, own, *out):
    own[...] = keep[0].astype(f32) + got[0].astype(f32)
    for s in range(1, 4):
        out[s - 1][...] = (keep[s].astype(f32) + got[s].astype(f32)).astype(bf16)


def total_kernel(flag, own, state, a, b, d, out):
    base = jnp.where(flag[0] == 0, state[...].astype(f32), 0.0)
    out[...] = (
        own[...] + base + (a[...].astype(f32) + b[...].astype(f32) + d[...].astype(f32))
    ).astype(bf16)


def join_kernel(flag, a, b, out):
    out[...] = (a[...].astype(f32) + b[...].astype(f32)).astype(bf16)


def join_fresh_kernel(flag, a, b, fresh, out):
    joined = (a[...].astype(f32) + b[...].astype(f32)).astype(bf16)
    out[...] = jnp.where(flag[1] == 0, fresh[...], joined)


def local(kernel, scalars, values, outs, scratch=(), name=None):
    vmem = pl.BlockSpec(memory_space=pltpu.VMEM)
    values = [pltpu.with_memory_space_constraint(v, pltpu.VMEM) for v in values]
    single = not isinstance(outs, list)
    result = pl.pallas_call(
        kernel,
        in_specs=[pl.BlockSpec(memory_space=pltpu.SMEM)] * len(scalars) + [vmem] * len(values),
        out_specs=vmem if single else [vmem] * len(outs),
        out_shape=outs,
        scratch_shapes=list(scratch),
        compiler_params=pltpu.CompilerParams(vmem_limit_bytes=20 * 1024 * 1024),
        name=name,
    )(*scalars, *values)
    return result


def out_vmem(shape, dtype):
    return pltpu.VMEM(shape, dtype)


def call_mlp(place, mine, theirs, gain, weights):
    tokens = mine[0].shape[0]
    return local(
        mlp_kernel, [place], [*mine, *theirs, gain, *weights],
        [
            out_vmem((4, tokens, 512), bf16),
            out_vmem((4, tokens, 512), bf16),
            out_vmem((tokens // 32, 640), f32),
        ],
        [pltpu.VMEM((tokens, 4096), bf16)], "mlp",
    )


def call_last(place, mine, theirs, gain, weights, before):
    tokens = mine[0].shape[0]
    rows = sum(b.shape[0] for b in before) + tokens // 32
    return local(
        functools.partial(last_kernel, len(before)), [place],
        [*mine, *theirs, gain, *weights, *before],
        out_vmem((16, rows, 256), f32),
        [pltpu.VMEM((tokens, 4096), bf16)], "last_mlp",
    )


def head_kernel(place, chosen_ref, all_ref, gain_ref, head_ref, out_ref):
    total = squares = None
    for m in range(16):
        cols = slice(m * 256, (m + 1) * 256)
        v = jnp.concatenate([all_ref[0, m], all_ref[1, m]], axis=0)
        now = jnp.dot(v, head_ref[cols, :], preferred_element_type=f32)
        total = now if total is None else total + now
        plain = v.astype(f32) / gain_ref[:, cols]
        plain = plain * plain
        plain = plain[:, :128] + plain[:, 128:]
        squares = plain if squares is None else squares + plain
    factor = lax.rsqrt(jnp.sum(squares, axis=1, keepdims=True) / 4096 + final_eps)
    here = place[0]
    mine = jnp.concatenate([all_ref[0, here], all_ref[1, here]], axis=0).astype(f32) * factor
    scores = lax.dot_general(
        total * factor, mine, (((1,), (1,)), ((), ())),
        precision=lax.Precision.HIGHEST, preferred_element_type=f32,
    )
    skew = scores - scores.T
    chosen = chosen_ref[...]
    count = skew.shape[0]
    hot = (lax.broadcasted_iota(jnp.int32, (chosen.shape[0], count), 1) == chosen).astype(f32)
    rows = jnp.dot(hot, skew, precision=lax.Precision.HIGHEST, preferred_element_type=f32)
    out_ref[...] = lax.dot_general(
        rows, hot, (((1,), (1,)), ((), ())),
        precision=lax.Precision.HIGHEST, preferred_element_type=f32,
    )


def head_part(place, chosen, everyone, gain, head):
    vmem = pl.BlockSpec(memory_space=pltpu.VMEM)
    return pl.pallas_call(
        head_kernel,
        in_specs=[pl.BlockSpec(memory_space=pltpu.SMEM)] + [vmem] * 4,
        out_specs=vmem,
        out_shape=jax.ShapeDtypeStruct((chosen.shape[0], chosen.shape[0]), f32),
        name="head",
    )(place, chosen, everyone, gain, head)


def per_device(
    token_ids, members, owners, embed_table, norm_gain, gate_weight, up_weight, down_weight,
    final_gain, head_weight,
):
    section = lax.axis_index("section")
    mp = lax.axis_index("mp")
    dp = lax.axis_index("dp")
    x, y, c = mp // 4, (mp // 2) % 2, mp % 2
    place = jnp.stack([x, c]).astype(jnp.int32)
    weights = (gate_weight, up_weight, down_weight)
    flat = token_ids.reshape(-1, 1) - section * embed_table.shape[1]
    block = flat.shape[0] // BLOCKS

    def fresh(index):
        part = embed_part(flat[index * block : (index + 1) * block], embed_table)
        pieces = [to_first(part, z) for z in (1, 3, 2)]
        own = part + pieces[0] + pieces[1] + pieces[2]
        peer = other_y(own)
        return jnp.where(
            y == 0, jnp.concatenate([own, peer], axis=1), jnp.concatenate([peer, own], axis=1)
        )

    flags = jnp.stack([y, section]).astype(jnp.int32)
    blocks = [fresh(i) for i in range(BLOCKS)]
    size = (block, 512)
    states = [None] * STREAMS
    sums_state, sums_hidden = {}, {}
    rounds = BLOCKS // STREAMS
    ticks = rounds + 3
    for tick in range(ticks):
        for stream in range(STREAMS):
            state = blocks[stream] if tick == 0 else states[stream]
            which = (tick - 3) * STREAMS + stream
            if tick >= 3:
                sums_state[which] = mean_tokens(state.astype(f32))
            mine = [state] + [along_x(state, s) for s in (1, 2, 3)]
            theirs = [other_core(m) for m in mine]
            if which == BLOCKS - 1:
                before = [sums_hidden[i] for i in range(BLOCKS - 1)]
                terms = call_last(place, mine, theirs, norm_gain, weights, before)
                continue
            send, keep, pooled = call_mlp(place, mine, theirs, norm_gain, weights)
            if tick >= 3:
                sums_hidden[which] = pooled
            if tick == ticks - 1:
                continue
            own, *halves = local(
                halves_kernel, [], [keep, other_core(send)],
                [out_vmem(size, f32)] + [out_vmem(size, bf16)] * 3, (), "halves",
            )
            arrived = [along_x(halves[s - 1], s) for s in (2, 1, 3)]
            total = local(
                total_kernel, [flags], [own, state, *arrived], out_vmem(size, bf16), (), "total"
            )
            parts = [onward(total, 0), onward(total, 1)]
            if tick + 1 < rounds:
                parts.append(blocks[(tick + 1) * STREAMS + stream])
                kernel = join_fresh_kernel
            else:
                kernel = join_kernel
            states[stream] = local(kernel, [flags], parts, out_vmem(size, bf16), (), "join")

    pieces = lax.all_to_all(terms, "mp", 0, 0, tiled=True)
    base = jnp.concatenate([sums_state[i] for i in range(BLOCKS)], axis=0)
    pooled = jnp.sum(pieces, axis=0) + jnp.where(y == 0, base[:, :256], base[:, 256:])
    gain_here = lax.dynamic_slice_in_dim(final_gain, mp * 256, 256)
    value = (pooled * gain_here[None, :]).astype(bf16)
    everyone = lax.all_to_all(
        jnp.broadcast_to(value, (32, *value.shape)), ("dp", "mp"), 0, 0, tiled=True
    ).reshape(2, 16, *value.shape)

    prompts = owners.shape[0]
    here = prompts // 2
    slots = dp * here + jnp.arange(here, dtype=jnp.int32)
    match = (owners[None, :] == slots[:, None]).astype(jnp.int32)
    hit = match[:, :, None] * members.reshape(prompts, GROUP)[None]
    chosen = jnp.sum(hit, axis=1).reshape(here * GROUP, 1)
    tile = head_part(
        jnp.reshape(mp, (1,)).astype(jnp.int32), chosen, everyone, final_gain[None], head_weight
    )
    rows = GROUP // 4
    parts = jnp.stack([tile[p * GROUP : (p + 1) * GROUP, p * GROUP : (p + 1) * GROUP] for p in range(here)])
    parts = jnp.swapaxes(parts.reshape(here, 4, rows, GROUP), 0, 1).reshape(4, 1, 1, -1)
    parts = jnp.broadcast_to(parts, (4, 16, 1, parts.shape[-1])).reshape(64, 1, -1)
    got = lax.all_to_all(parts, ("section", "mp"), 0, 0, tiled=True)
    skew = jnp.sum(got[48:], axis=(0, 1))
    return jax.nn.sigmoid(skew).reshape(here, rows, GROUP)


def solution(mesh):
    placed = (
        P("dp", None),
        P(),
        P(),
        P("mp", "section"),
        P("section", None),
        P("section", None, "mp"),
        P("section", None, "mp"),
        P("section", None, "mp"),
        P(),
        P(None, "mp"),
    )
    return jax.shard_map(
        per_device, mesh=mesh, in_specs=placed, out_specs=P("dp", "section", None), check_vma=False
    )
```

```python
import functools

import jax
import jax.numpy as jnp
from jax import lax
from jax.experimental import pallas as pl
from jax.experimental.pallas import tpu as pltpu
from jax.sharding import PartitionSpec as P

GROUP = 8
BLOCKS = 2
AXES = ("dp", "section", "mp")

norm_eps = 1e-05
final_eps = 1e-06
bf16 = jnp.bfloat16
f32 = jnp.float32


def moved(value, target):
    pairs = []
    for dp in range(2):
        for z in range(4):
            for x in range(4):
                for y in range(2):
                    for c in range(2):
                        to = target(dp, z, x, y, c)
                        if to is not None:
                            d, s, a, b, e = to
                            pairs.append(
                                (dp * 64 + z * 16 + x * 4 + y * 2 + c, d * 64 + s * 16 + a * 4 + b * 2 + e)
                            )
    return lax.ppermute(value, AXES, pairs)


def along_x(value, shift):
    return moved(value, lambda d, z, x, y, c: (d, z, (x + shift) % 4, y, c))


def other_core(value):
    return moved(value, lambda d, z, x, y, c: (d, z, x, y, 1 - c))


def other_dp(value):
    return moved(value, lambda d, z, x, y, c: (1 - d, z, x, y, c))


def other_y(value):
    return moved(value, lambda d, z, x, y, c: (1 - d, z, x, 1 - y, c))


def to_first(value, source):
    return moved(value, lambda d, z, x, y, c: (d, 0, x, y, c) if z == source else None)


def onward(value, flip):
    return moved(value, lambda d, z, x, y, c: (d ^ flip, z + 1, x, y ^ flip, c) if z < 3 else None)


def nt_dot(a, b):
    return lax.dot_general(a, b, (((1,), (1,)), ((), ())), preferred_element_type=f32)


def embed_kernel(width, ids_ref, table_ref, *refs):
    outs, (held, sems) = refs[:-2], refs[-2:]
    rows = ids_ref.shape[0]
    steps = table_ref.shape[1] // width

    def copy(step):
        cols = pl.ds(pl.multiple_of(step * width, width), width)
        return pltpu.make_async_copy(table_ref.at[:, cols], held.at[:, cols], sems.at[step])

    def begin(step, carry):
        copy(step).start()
        return carry

    lax.fori_loop(0, steps, begin, 0)

    def one(step, acc):
        copy(step).wait()
        start = pl.multiple_of(step * width, width)
        hot = lax.broadcasted_iota(jnp.int32, (rows, width), 1) == ids_ref[...] - start
        return acc + nt_dot(hot.astype(f32).astype(bf16), held[:, pl.ds(start, width)])

    acc = lax.fori_loop(0, steps, one, jnp.zeros((rows, table_ref.shape[0]), f32))
    count = rows // len(outs)
    for i, out in enumerate(outs):
        out[...] = acc[i * count : (i + 1) * count].astype(bf16)


def in_hbm(value):
    return pltpu.with_memory_space_constraint(value, pltpu.HBM)


def in_vmem(value):
    return pltpu.with_memory_space_constraint(value, pltpu.VMEM)


VMEM_SPEC = pl.BlockSpec(memory_space=pltpu.VMEM)
HBM_SPEC = pl.BlockSpec(memory_space=pltpu.HBM)
SMEM_SPEC = pl.BlockSpec(memory_space=pltpu.SMEM)


def embed_parts(ids, table, count):
    width = 1024
    rows = ids.shape[0] // count
    return pl.pallas_call(
        functools.partial(embed_kernel, width),
        in_specs=[VMEM_SPEC, HBM_SPEC],
        out_specs=[VMEM_SPEC] * count,
        out_shape=[pltpu.VMEM((rows, table.shape[0]), bf16)] * count,
        scratch_shapes=[
            pltpu.VMEM(table.shape, bf16),
            pltpu.SemaphoreType.DMA((table.shape[1] // width,)),
        ],
        compiler_params=pltpu.CompilerParams(vmem_limit_bytes=24 * 1024 * 1024),
        name="embed",
    )(in_vmem(ids), in_hbm(table))


def load_kernel(count, after, *refs):
    sources, places, sems = refs[:count], refs[count : 2 * count], refs[-1]
    copies = []
    for i, (source, place) in enumerate(zip(sources, places)):
        rows = source.shape[1] // 4
        for k in range(4):
            where = (0, pl.ds(k * rows, rows))
            copies.append(
                pltpu.make_async_copy(source.at[where], place.at[where], sems.at[4 * i + k])
            )
    for copy in copies:
        copy.start()
    for copy in copies:
        copy.wait()


def loaded(after, *arrays):
    count = len(arrays)
    return pl.pallas_call(
        functools.partial(load_kernel, count),
        in_specs=[VMEM_SPEC] + [HBM_SPEC] * count,
        out_specs=[VMEM_SPEC] * count,
        out_shape=[pltpu.VMEM(a.shape, a.dtype) for a in arrays],
        scratch_shapes=[pltpu.SemaphoreType.DMA((4 * count,))],
        compiler_params=pltpu.CompilerParams(vmem_limit_bytes=1024 * 1024),
        name="load",
    )(in_vmem(after), *[in_hbm(a) for a in arrays])


def prepare(x, c, chunks, gain_ref, scaled_ref, inverse_ref):
    def one(step, carry):
        rows = pl.ds(pl.multiple_of(step * 32, 32), 32)
        squares = None
        for shift in range(4):
            base = lax.rem(x + 4 - shift, 4) * 1024
            for ref, core in ((chunks[shift], c), (chunks[4 + shift], 1 - c)):
                for y in range(2):
                    block = ref[rows, y * 256 : (y + 1) * 256].astype(f32)
                    off = pl.multiple_of(base + y * 512 + core * 256, 256)
                    scaled_ref[rows, pl.ds(off, 256)] = (
                        block * gain_ref[:, pl.ds(off, 256)]
                    ).astype(bf16)
                    part = block[:, :128] * block[:, :128] + block[:, 128:] * block[:, 128:]
                    squares = part if squares is None else squares + part
        total = jnp.sum(squares, axis=1, keepdims=True)
        inverse_ref[rows, :] = jnp.broadcast_to(lax.rsqrt(total / 4096 + norm_eps), (32, 128))
        return carry

    lax.fori_loop(0, chunks[0].shape[0] // 32, one, 0)


def hidden_units(scaled, wg, wu, inverse_ref, gate_ref, up_ref):
    def one(k, carry):
        cols = pl.ds(pl.multiple_of(k * 1024, 1024), 1024)
        part = scaled[:, cols]
        gate = jnp.dot(part, wg[0, cols, :], preferred_element_type=f32)
        up = jnp.dot(part, wu[0, cols, :], preferred_element_type=f32)
        gate_ref[...] = jnp.where(k == 0, gate, gate_ref[...] + gate)
        up_ref[...] = jnp.where(k == 0, up, up_ref[...] + up)
        return carry

    lax.fori_loop(0, 4, one, 0)
    inverse = inverse_ref[:, :1]
    gate = gate_ref[...] * inverse
    return gate / (1.0 + jnp.exp(-gate)) * (up_ref[...] * inverse)


def mean_tokens(value):
    rows, cols = value.shape
    return jnp.sum(value.reshape(rows // 32, 32, cols), axis=1) * (1.0 / 32)


def mlp_kernel(pool, place, *refs):
    chunks, (gain, wg, wu, wd) = refs[:8], refs[8:12]
    send, keep = refs[12:14]
    scaled, inverse, gate, up = refs[-4:]
    x, c = place[0], place[1]
    prepare(x, c, chunks, gain, scaled, inverse)
    hidden = hidden_units(scaled, wg, wu, inverse, gate, up)
    if pool:
        refs[14][...] = mean_tokens(hidden)
        refs[15][...] = mean_tokens(chunks[0][...].astype(f32))
    rounded = hidden.astype(bf16)
    first = c == 0

    def one(s, carry):
        rows = pl.multiple_of(lax.rem(x + s, 4) * 1024, 1024)
        term = nt_dot(rounded, wd[0, pl.ds(rows, 1024), :])
        for y in range(2):
            a = term[:, y * 512 : y * 512 + 256]
            b = term[:, y * 512 + 256 : y * 512 + 512]
            cols = slice(y * 256, (y + 1) * 256)
            keep[s, :, cols] = jnp.where(first, a, b).astype(bf16)
            send[s, :, cols] = jnp.where(first, b, a).astype(bf16)
        return carry

    lax.fori_loop(0, 4, one, 0)


def last_kernel(count, place, *refs):
    chunks, (gain, wg, wu, wd) = refs[:8], refs[8:12]
    before = refs[12 : 12 + count]
    out, base = refs[12 + count : 14 + count]
    scaled, inverse, gate, up = refs[-4:]
    x, c = place[0], place[1]
    prepare(x, c, chunks, gain, scaled, inverse)
    hidden = hidden_units(scaled, wg, wu, inverse, gate, up)
    base[...] = mean_tokens(chunks[0][...].astype(f32))
    every = jnp.concatenate([ref[...] for ref in before] + [mean_tokens(hidden)], axis=0)
    high = every.astype(bf16)
    low = (every - high.astype(f32)).astype(bf16)
    rows = every.shape[0]
    stacked = jnp.concatenate([high, low], axis=0)

    def one(m, carry):
        term = nt_dot(stacked, wd[0, pl.ds(pl.multiple_of(m * 256, 256), 256), :])
        out[m] = term[:rows] + term[rows:]
        return carry

    lax.fori_loop(0, 16, one, 0)


def gathered_kernel(own, a, b, d, out):
    out[...] = (
        own[...].astype(f32) + a[...].astype(f32) + (b[...].astype(f32) + d[...].astype(f32))
    ).astype(bf16)


def by_y(flag, own, peer):
    first = flag[2] == 0
    low, high = own[...].astype(f32), peer[...].astype(f32)
    return jnp.concatenate(
        [jnp.where(first, low, high), jnp.where(first, high, low)], axis=1
    )


def fresh_kernel(flag, own, peer, out):
    out[...] = by_y(flag, own, peer).astype(bf16)


def halves_kernel(keep, got, own, *out):
    own[...] = keep[0].astype(f32) + got[0].astype(f32)
    for s in range(1, 4):
        out[s - 1][...] = (keep[s].astype(f32) + got[s].astype(f32)).astype(bf16)


def total_kernel(flag, own, state, a, b, d, out):
    base = jnp.where(flag[2] == 0, state[...].astype(f32), 0.0)
    out[...] = (
        own[...] + base + (a[...].astype(f32) + b[...].astype(f32) + d[...].astype(f32))
    ).astype(bf16)


def join_kernel(flag, a, b, out):
    out[...] = (a[...].astype(f32) + b[...].astype(f32)).astype(bf16)


def join_fresh_kernel(flag, a, b, own, peer, out):
    joined = a[...].astype(f32) + b[...].astype(f32)
    out[...] = jnp.where(flag[3] == 0, by_y(flag, own, peer), joined).astype(bf16)


def local(kernel, scalars, values, outs, scratch=(), name=None):
    single = not isinstance(outs, list)
    return pl.pallas_call(
        kernel,
        in_specs=[SMEM_SPEC] * len(scalars) + [VMEM_SPEC] * len(values),
        out_specs=VMEM_SPEC if single else [VMEM_SPEC] * len(outs),
        out_shape=outs,
        scratch_shapes=list(scratch),
        compiler_params=pltpu.CompilerParams(vmem_limit_bytes=20 * 1024 * 1024),
        name=name,
    )(*scalars, *[in_vmem(v) for v in values])


def out_vmem(shape, dtype):
    return pltpu.VMEM(shape, dtype)


def mlp_scratch(tokens):
    return [
        pltpu.VMEM((tokens, 4096), bf16),
        pltpu.VMEM((tokens, 128), f32),
        pltpu.VMEM((tokens, 640), f32),
        pltpu.VMEM((tokens, 640), f32),
    ]


def call_mlp(place, mine, theirs, gain, weights, pool):
    tokens = mine[0].shape[0]
    outs = [out_vmem((4, tokens, 512), bf16)] * 2
    if pool:
        outs += [out_vmem((tokens // 32, 640), f32), out_vmem((tokens // 32, 512), f32)]
    return local(
        functools.partial(mlp_kernel, pool), [place], [*mine, *theirs, gain, *weights], outs,
        mlp_scratch(tokens), "mlp",
    )


def call_last(place, mine, theirs, gain, weights, before):
    tokens = mine[0].shape[0]
    rows = sum(b.shape[0] for b in before) + tokens // 32
    return local(
        functools.partial(last_kernel, len(before)), [place],
        [*mine, *theirs, gain, *weights, *before],
        [out_vmem((16, rows, 256), f32), out_vmem((tokens // 32, 512), f32)],
        mlp_scratch(tokens), "last_mlp",
    )


def head_kernel(place, chosen_ref, all_ref, gain_ref, head_ref, out_ref):
    total = squares = None
    for m in range(16):
        cols = slice(m * 256, (m + 1) * 256)
        side = (m // 2) % 2
        v = jnp.concatenate([all_ref[side, m], all_ref[1 - side, m]], axis=0)
        now = jnp.dot(v, head_ref[cols, :], preferred_element_type=f32)
        total = now if total is None else total + now
        plain = v.astype(f32) / gain_ref[:, cols]
        plain = plain * plain
        plain = plain[:, :128] + plain[:, 128:]
        squares = plain if squares is None else squares + plain
    factor = lax.rsqrt(jnp.sum(squares, axis=1, keepdims=True) / 4096 + final_eps)
    here = place[0]
    side = lax.rem(here // 2, 2)
    mine = jnp.concatenate([all_ref[side, here], all_ref[1 - side, here]], axis=0)
    mine = mine.astype(f32) * factor
    scores = lax.dot_general(
        total * factor, mine, (((1,), (1,)), ((), ())),
        precision=lax.Precision.HIGHEST, preferred_element_type=f32,
    )
    skew = scores - scores.T
    chosen = chosen_ref[...]
    count = skew.shape[0]
    hot = (lax.broadcasted_iota(jnp.int32, (chosen.shape[0], count), 1) == chosen).astype(f32)
    rows = jnp.dot(hot, skew, precision=lax.Precision.HIGHEST, preferred_element_type=f32)
    out_ref[...] = lax.dot_general(
        rows, hot, (((1,), (1,)), ((), ())),
        precision=lax.Precision.HIGHEST, preferred_element_type=f32,
    )


def head_part(place, chosen, everyone, gain, head):
    vmem = pl.BlockSpec(memory_space=pltpu.VMEM)
    return pl.pallas_call(
        head_kernel,
        in_specs=[pl.BlockSpec(memory_space=pltpu.SMEM)] + [vmem] * 4,
        out_specs=vmem,
        out_shape=jax.ShapeDtypeStruct((chosen.shape[0], chosen.shape[0]), f32),
        name="head",
    )(place, chosen, everyone, gain, head)


def per_device(
    token_ids, members, owners, embed_table, norm_gain, gate_weight, up_weight, down_weight,
    final_gain, head_weight,
):
    section = lax.axis_index("section")
    mp = lax.axis_index("mp")
    dp = lax.axis_index("dp")
    x, y, c = mp // 4, (mp // 2) % 2, mp % 2
    place = jnp.stack([x, c, y, section]).astype(jnp.int32)
    ids = jnp.where(y == 0, token_ids, other_dp(token_ids))
    flat = ids.reshape(-1, 1) - section * embed_table.shape[1]
    parts = embed_parts(flat, embed_table, BLOCKS)
    weights = loaded(parts[0], gate_weight, up_weight, down_weight)
    size = (parts[0].shape[0], 512)
    half = (parts[0].shape[0], 256)

    fresh = []
    for part in parts:
        pieces = [to_first(part, z) for z in (1, 3, 2)]
        own = local(gathered_kernel, [], [part, *pieces], out_vmem(half, bf16), (), "gathered")
        fresh.append((own, other_y(own)))
    state = local(fresh_kernel, [place], fresh[0], out_vmem(size, bf16), (), "fresh")
    sums_state, sums_hidden = [], []
    ticks = BLOCKS + 3
    for tick in range(ticks):
        mine = [state] + [along_x(state, s) for s in (1, 3, 2)]
        mine = [mine[i] for i in (0, 1, 3, 2)]
        theirs = [other_core(m) for m in mine]
        if tick == ticks - 1:
            terms, base = call_last(place, mine, theirs, norm_gain, weights, sums_hidden)
            sums_state.append(base)
            break
        send, keep, *pooled = call_mlp(place, mine, theirs, norm_gain, weights, tick >= 3)
        if tick >= 3:
            sums_hidden.append(pooled[0])
            sums_state.append(pooled[1])
        own, *halves = local(
            halves_kernel, [], [keep, other_core(send)],
            [out_vmem(size, f32)] + [out_vmem(size, bf16)] * 3, (), "halves",
        )
        arrived = [along_x(halves[s - 1], s) for s in (1, 3, 2)]
        total = local(
            total_kernel, [place], [own, state, *arrived], out_vmem(size, bf16), (), "total"
        )
        ahead = [onward(total, 0), onward(total, 1)]
        kernel = join_kernel
        if tick + 1 < BLOCKS:
            ahead += fresh[tick + 1]
            kernel = join_fresh_kernel
        state = local(kernel, [place], ahead, out_vmem(size, bf16), (), "join")

    groups = [[(g ^ ((m // 2) % 2)) * 16 + m for m in range(16)] for g in range(2)]
    pieces = lax.all_to_all(
        terms, ("dp", "mp"), 0, 0, tiled=True, axis_index_groups=groups
    )
    base = jnp.concatenate(sums_state, axis=0)
    pooled = jnp.sum(pieces, axis=0) + jnp.where(y == 0, base[:, :256], base[:, 256:])
    gain_here = lax.dynamic_slice_in_dim(final_gain, mp * 256, 256)
    value = (pooled * gain_here[None, :]).astype(bf16)
    everyone = lax.all_to_all(
        jnp.broadcast_to(value, (32, *value.shape)), ("dp", "mp"), 0, 0, tiled=True
    ).reshape(2, 16, *value.shape)

    prompts = owners.shape[0]
    here = prompts // 2
    slots = dp * here + jnp.arange(here, dtype=jnp.int32)
    match = (owners[None, :] == slots[:, None]).astype(jnp.int32)
    hit = match[:, :, None] * members.reshape(prompts, GROUP)[None]
    chosen = jnp.sum(hit, axis=1).reshape(here * GROUP, 1)
    tile = head_part(
        jnp.reshape(mp, (1,)).astype(jnp.int32), chosen, everyone, final_gain[None], head_weight
    )
    rows = GROUP // 4
    parts = jnp.stack(
        [tile[p * GROUP : (p + 1) * GROUP, p * GROUP : (p + 1) * GROUP] for p in range(here)]
    )
    parts = jnp.swapaxes(parts.reshape(here, 4, rows, GROUP), 0, 1).reshape(4, here * rows, GROUP)
    parts = jnp.pad(parts, ((0, 0), (0, 8 - here * rows), (0, 128 - GROUP)))
    parts = jnp.broadcast_to(parts[None, :, None], (2, 4, 16, 8, 128)).reshape(128, 8, 128)
    got = lax.all_to_all(parts, AXES, 0, 0, tiled=True).reshape(2, 4, 16, 8, 128)
    skew = jnp.sum(jnp.where(dp == 0, got[0, 3], got[1, 3]), axis=0)[: here * rows, :GROUP]
    return jax.nn.sigmoid(skew).reshape(here, rows, GROUP)


def solution(mesh):
    placed = (
        P("dp", None),
        P(),
        P(),
        P("mp", "section"),
        P("section", None),
        P("section", None, "mp"),
        P("section", None, "mp"),
        P("section", None, "mp"),
        P(),
        P(None, "mp"),
    )
    return jax.shard_map(
        per_device, mesh=mesh, in_specs=placed, out_specs=P("dp", "section", None), check_vma=False
    )
```

```python
import functools

import jax
import jax.numpy as jnp
from jax import lax
from jax.experimental import pallas as pl
from jax.experimental.pallas import tpu as pltpu
from jax.sharding import PartitionSpec as P


GROUP = 8
BLOCKS = 2
STREAMS = 1
AXES = ("dp", "section", "mp")

norm_eps = 1e-05
final_eps = 1e-06
bf16 = jnp.bfloat16
f32 = jnp.float32


def moved(value, target):
    pairs = []
    for dp in range(2):
        for z in range(4):
            for x in range(4):
                for y in range(2):
                    for c in range(2):
                        to = target(dp, z, x, y, c)
                        if to is not None:
                            d, s, a, b, e = to
                            pairs.append(
                                (dp * 64 + z * 16 + x * 4 + y * 2 + c, d * 64 + s * 16 + a * 4 + b * 2 + e)
                            )
    return lax.ppermute(value, AXES, pairs)


def along_x(value, shift):
    return moved(value, lambda d, z, x, y, c: (d, z, (x + shift) % 4, y, c))


def other_core(value):
    return moved(value, lambda d, z, x, y, c: (d, z, x, y, 1 - c))


def other_dp(value):
    return moved(value, lambda d, z, x, y, c: (1 - d, z, x, y, c))


def other_y(value):
    return moved(value, lambda d, z, x, y, c: (1 - d, z, x, 1 - y, c))


def along_sections(value, shift):
    return moved(value, lambda d, z, x, y, c: (d, (z + shift) % 4, x, y, c))


def onward(value, flip):
    return moved(value, lambda d, z, x, y, c: (d ^ flip, (z + 1) % 4, x, y ^ flip, c))


def nt_dot(a, b):
    return lax.dot_general(a, b, (((1,), (1,)), ((), ())), preferred_element_type=f32)


def embed_kernel(width, first, place, ids_ref, table_ref, out, held, sems):
    rows = out.shape[0]
    ids = ids_ref[first : first + rows, :]
    steps = table_ref.shape[1] // width

    def copy(step):
        cols = pl.ds(pl.multiple_of(step * width, width), width)
        return pltpu.make_async_copy(table_ref.at[:, cols], held.at[:, cols], sems.at[step])

    def begin(step, carry):
        copy(step).start()
        return carry

    lax.fori_loop(0, steps, begin, 0)

    def one(step, acc):
        copy(step).wait()
        start = pl.multiple_of(step * width, width)
        hot = lax.broadcasted_iota(jnp.int32, (rows, width), 1) == ids - start
        return acc + nt_dot(hot.astype(f32).astype(bf16), held[:, pl.ds(start, width)])

    acc = lax.fori_loop(0, steps, one, jnp.zeros((rows, table_ref.shape[0]), f32))
    out[...] = acc.astype(bf16)


def cost(products):
    return pl.CostEstimate(flops=2 * products, bytes_accessed=0, transcendentals=0)


def in_hbm(value):
    return pltpu.with_memory_space_constraint(value, pltpu.HBM)


def in_vmem(value):
    return pltpu.with_memory_space_constraint(value, pltpu.VMEM)


VMEM_SPEC = pl.BlockSpec(memory_space=pltpu.VMEM)
HBM_SPEC = pl.BlockSpec(memory_space=pltpu.HBM)
SMEM_SPEC = pl.BlockSpec(memory_space=pltpu.SMEM)


def embed_part(place, ids, first, rows, table):
    width = 1024
    return pl.pallas_call(
        functools.partial(embed_kernel, width, first),
        in_specs=[SMEM_SPEC, VMEM_SPEC, HBM_SPEC],
        out_specs=VMEM_SPEC,
        out_shape=pltpu.VMEM((rows, table.shape[0]), bf16),
        scratch_shapes=[
            pltpu.VMEM(table.shape, bf16),
            pltpu.SemaphoreType.DMA((table.shape[1] // width,)),
        ],
        compiler_params=pltpu.CompilerParams(vmem_limit_bytes=14 * 1024 * 1024),
        cost_estimate=cost(rows * table.size),
        name="embed",
    )(place, in_vmem(ids), in_hbm(table))


def load_kernel(count, after, *refs):
    sources, places, sems = refs[:count], refs[count : 2 * count], refs[-1]
    copies = []
    for i, (source, place) in enumerate(zip(sources, places)):
        rows = source.shape[1] // 4
        for k in range(4):
            where = (0, pl.ds(k * rows, rows))
            copies.append(
                pltpu.make_async_copy(source.at[where], place.at[where], sems.at[4 * i + k])
            )
    for copy in copies:
        copy.start()
    for copy in copies:
        copy.wait()


def loaded(after, *arrays):
    count = len(arrays)
    return pl.pallas_call(
        functools.partial(load_kernel, count),
        in_specs=[VMEM_SPEC] + [HBM_SPEC] * count,
        out_specs=[VMEM_SPEC] * count,
        out_shape=[pltpu.VMEM(a.shape, a.dtype) for a in arrays],
        scratch_shapes=[pltpu.SemaphoreType.DMA((4 * count,))],
        compiler_params=pltpu.CompilerParams(vmem_limit_bytes=1024 * 1024),
        name="load",
    )(in_vmem(after), *[in_hbm(a) for a in arrays])


def prepare(x, c, chunks, gain_ref, scaled_ref, inverse_ref):
    def one(step, carry):
        rows = pl.ds(pl.multiple_of(step * 32, 32), 32)
        squares = None
        for shift in range(4):
            base = lax.rem(x + 4 - shift, 4) * 1024
            for ref, core in ((chunks[shift], c), (chunks[4 + shift], 1 - c)):
                for y in range(2):
                    block = ref[rows, y * 256 : (y + 1) * 256].astype(f32)
                    off = pl.multiple_of(base + y * 512 + core * 256, 256)
                    scaled_ref[rows, pl.ds(off, 256)] = (
                        block * gain_ref[:, pl.ds(off, 256)]
                    ).astype(bf16)
                    part = block[:, :128] * block[:, :128] + block[:, 128:] * block[:, 128:]
                    squares = part if squares is None else squares + part
        total = jnp.sum(squares, axis=1, keepdims=True)
        inverse_ref[rows, :] = jnp.broadcast_to(lax.rsqrt(total / 4096 + norm_eps), (32, 128))
        return carry

    lax.fori_loop(0, chunks[0].shape[0] // 32, one, 0)


def hidden_units(scaled, wg, wu, inverse_ref, gate_ref, up_ref, wait=None):
    def one(k, carry):
        if wait is not None:
            wait(0, k)
            wait(1, k)
        cols = pl.ds(pl.multiple_of(k * 1024, 1024), 1024)
        part = scaled[:, cols]
        gate = jnp.dot(part, wg[0, cols, :], preferred_element_type=f32)
        up = jnp.dot(part, wu[0, cols, :], preferred_element_type=f32)
        gate_ref[...] = jnp.where(k == 0, gate, gate_ref[...] + gate)
        up_ref[...] = jnp.where(k == 0, up, up_ref[...] + up)
        return carry

    lax.fori_loop(0, 4, one, 0)
    inverse = inverse_ref[:, :1]
    gate = gate_ref[...] * inverse
    return gate / (1.0 + jnp.exp(-gate)) * (up_ref[...] * inverse)


def mean_tokens(value):
    rows, cols = value.shape
    return jnp.sum(value.reshape(rows // 32, 32, cols), axis=1) * (1.0 / 32)


def mlp_kernel(pool, place, *refs):
    chunks, (gain, wg, wu, wd) = refs[:8], refs[8:12]
    send, keep = refs[12:14]
    scaled, inverse, gate, up = refs[-4:]
    x, c = place[0], place[1]
    prepare(x, c, chunks, gain, scaled, inverse)
    hidden = hidden_units(scaled, wg, wu, inverse, gate, up)
    if pool:
        refs[14][...] = mean_tokens(hidden)
        refs[15][...] = mean_tokens(chunks[0][...].astype(f32))
    rounded = hidden.astype(bf16)
    first = c == 0

    def one(s, carry):
        rows = pl.multiple_of(lax.rem(x + s, 4) * 1024, 1024)
        term = nt_dot(rounded, wd[0, pl.ds(rows, 1024), :])
        for y in range(2):
            a = term[:, y * 512 : y * 512 + 256]
            b = term[:, y * 512 + 256 : y * 512 + 512]
            cols = slice(y * 256, (y + 1) * 256)
            keep[s, :, cols] = jnp.where(first, a, b).astype(bf16)
            send[s, :, cols] = jnp.where(first, b, a).astype(bf16)
        return carry

    lax.fori_loop(0, 4, one, 0)


def last_kernel(count, place, *refs):
    chunks, gain, before, far = refs[:8], refs[8], refs[9 : 9 + count], refs[9 + count : 12 + count]
    out, base = refs[12 + count : 14 + count]
    held, sems = refs[-8:-5], refs[-5]
    scaled, inverse, gate, up = refs[-4:]

    def copy(kind, k):
        rows = pl.ds(pl.multiple_of(k * 1024, 1024), 1024)
        return pltpu.make_async_copy(
            far[kind].at[0, rows, :], held[kind].at[0, rows, :], sems.at[kind * 4 + k]
        )

    def begin(k, carry):
        copy(0, k).start()
        copy(1, k).start()
        return carry

    def begin_down(k, carry):
        copy(2, k).start()
        return carry

    lax.fori_loop(0, 4, begin, 0)
    lax.fori_loop(0, 4, begin_down, 0)
    prepare(place[0], place[1], chunks, gain, scaled, inverse)
    hidden = hidden_units(
        scaled, held[0], held[1], inverse, gate, up, lambda kind, k: copy(kind, k).wait()
    )
    base[...] = mean_tokens(chunks[0][...].astype(f32))
    every = jnp.concatenate([ref[...] for ref in before] + [mean_tokens(hidden)], axis=0)
    high = every.astype(bf16)
    low = (every - high.astype(f32)).astype(bf16)
    rows = every.shape[0]
    stacked = jnp.concatenate([high, low], axis=0)

    def one(k, carry):
        copy(2, k).wait()
        term = nt_dot(stacked, held[2][0, pl.ds(pl.multiple_of(k * 1024, 1024), 1024), :])
        term = term[:rows] + term[rows:]
        for m in range(4):
            out[4 * k + m] = term[:, m * 256 : (m + 1) * 256]
        return carry

    lax.fori_loop(0, 4, one, 0)


def gathered_kernel(own, a, b, d, out):
    out[...] = (
        own[...].astype(f32) + a[...].astype(f32) + (b[...].astype(f32) + d[...].astype(f32))
    ).astype(bf16)


def by_y(flag, own, peer):
    first = flag[2] == 0
    low, high = own[...].astype(f32), peer[...].astype(f32)
    return jnp.concatenate(
        [jnp.where(first, low, high), jnp.where(first, high, low)], axis=1
    )


def fresh_kernel(flag, own, peer, *out):
    whole = by_y(flag, own, peer).astype(bf16)
    rows = out[0].shape[0]
    for i, ref in enumerate(out):
        ref[...] = whole[i * rows : (i + 1) * rows]


def halves_kernel(keep, got, own, *out):
    own[...] = keep[0].astype(f32) + got[0].astype(f32)
    for s in range(1, 4):
        out[s - 1][...] = (keep[s].astype(f32) + got[s].astype(f32)).astype(bf16)


def total_kernel(flag, own, state, a, b, d, out):
    base = jnp.where(flag[2] == 0, state[...].astype(f32), 0.0)
    out[...] = (
        own[...] + base + (a[...].astype(f32) + b[...].astype(f32) + d[...].astype(f32))
    ).astype(bf16)


def join_kernel(flag, a, b, out):
    out[...] = (a[...].astype(f32) + b[...].astype(f32)).astype(bf16)


def join_fresh_kernel(flag, a, b, fresh, out):
    joined = (a[...].astype(f32) + b[...].astype(f32)).astype(bf16)
    out[...] = jnp.where(flag[3] == 0, fresh[...], joined)


def local(kernel, scalars, values, outs, scratch=(), limit=4, far=()):
    single = not isinstance(outs, list)
    return pl.pallas_call(
        kernel,
        in_specs=[SMEM_SPEC] * len(scalars) + [VMEM_SPEC] * len(values) + [HBM_SPEC] * len(far),
        out_specs=VMEM_SPEC if single else [VMEM_SPEC] * len(outs),
        out_shape=outs,
        scratch_shapes=list(scratch),
        compiler_params=pltpu.CompilerParams(vmem_limit_bytes=limit * 1024 * 1024),
    )(*scalars, *[in_vmem(v) for v in values], *[in_hbm(v) for v in far])


def out_vmem(shape, dtype):
    return pltpu.VMEM(shape, dtype)


def mlp_scratch(tokens):
    return [
        pltpu.VMEM((tokens, 4096), bf16),
        pltpu.VMEM((tokens, 128), f32),
        pltpu.VMEM((tokens, 640), f32),
        pltpu.VMEM((tokens, 640), f32),
    ]


def call_mlp(place, mine, theirs, gain, weights, pool):
    tokens = mine[0].shape[0]
    outs = [out_vmem((4, tokens, 512), bf16)] * 2
    if pool:
        outs += [out_vmem((tokens // 32, 640), f32), out_vmem((tokens // 32, 512), f32)]
    return local(
        functools.partial(mlp_kernel, pool), [place], [*mine, *theirs, gain, *weights], outs,
        mlp_scratch(tokens), 16,
    )


def call_last(place, mine, theirs, gain, far, before):
    tokens = mine[0].shape[0]
    rows = sum(b.shape[0] for b in before) + tokens // 32
    return local(
        functools.partial(last_kernel, len(before)), [place], [*mine, *theirs, gain, *before],
        [out_vmem((16, rows, 256), f32), out_vmem((tokens // 32, 512), f32)],
        [pltpu.VMEM((1, 4096, 640), bf16)] * 3
        + [pltpu.SemaphoreType.DMA((12,))]
        + mlp_scratch(tokens),
        28, far,
    )


def head_kernel(place, chosen_ref, all_ref, gain_ref, head_ref, out_ref):
    total = squares = None
    for m in range(16):
        cols = slice(m * 256, (m + 1) * 256)
        side = (m // 2) % 2
        v = jnp.concatenate([all_ref[side, m], all_ref[1 - side, m]], axis=0)
        now = jnp.dot(v, head_ref[cols, :], preferred_element_type=f32)
        total = now if total is None else total + now
        plain = v.astype(f32) / gain_ref[:, cols]
        plain = plain * plain
        plain = plain[:, :128] + plain[:, 128:]
        squares = plain if squares is None else squares + plain
    factor = lax.rsqrt(jnp.sum(squares, axis=1, keepdims=True) / 4096 + final_eps)
    here = place[0]
    side = lax.rem(here // 2, 2)
    mine = jnp.concatenate([all_ref[side, here], all_ref[1 - side, here]], axis=0)
    mine = mine.astype(f32) * factor
    scores = lax.dot_general(
        total * factor, mine, (((1,), (1,)), ((), ())),
        precision=lax.Precision.HIGHEST, preferred_element_type=f32,
    )
    skew = scores - scores.T
    chosen = chosen_ref[...]
    count = skew.shape[0]
    hot = (lax.broadcasted_iota(jnp.int32, (chosen.shape[0], count), 1) == chosen).astype(f32)
    half = out_ref.shape[0]
    rows = jnp.dot(hot[: 2 * half], skew, precision=lax.Precision.HIGHEST, preferred_element_type=f32)
    tile = lax.dot_general(
        rows, hot, (((1,), (1,)), ((), ())),
        precision=lax.Precision.HIGHEST, preferred_element_type=f32,
    )
    lane = lax.broadcasted_iota(jnp.int32, out_ref.shape, 1)
    out_ref[...] = jnp.where(lane < half, tile[:half], tile[half:])


def head_part(place, chosen, everyone, gain, head):
    vmem = pl.BlockSpec(memory_space=pltpu.VMEM)
    return pl.pallas_call(
        head_kernel,
        in_specs=[pl.BlockSpec(memory_space=pltpu.SMEM)] + [vmem] * 4,
        out_specs=vmem,
        out_shape=jax.ShapeDtypeStruct((GROUP, chosen.shape[0]), f32),
        name="head",
    )(place, chosen, everyone, gain, head)


def per_device(
    token_ids, members, owners, embed_table, norm_gain, gate_weight, up_weight, down_weight,
    final_gain, head_weight,
):
    section = lax.axis_index("section")
    mp = lax.axis_index("mp")
    dp = lax.axis_index("dp")
    x, y, c = mp // 4, (mp // 2) % 2, mp % 2
    place = jnp.stack([x, c, y, section]).astype(jnp.int32)
    ids = jnp.where(y == 0, token_ids, other_dp(token_ids))
    flat = ids.reshape(-1, 1) - section * embed_table.shape[1]
    together = flat.shape[0] * STREAMS // BLOCKS
    rounds = BLOCKS // STREAMS
    block = together // STREAMS
    size = (block, 512)

    def summed(part):
        pieces = []
        for z in (1, 3, 2):
            pieces.append(along_sections(part, z))
        return local(gathered_kernel, [], [part, *pieces], out_vmem(part.shape, bf16), ())

    def start_of(own):
        return local(fresh_kernel, [place], [own, other_y(own)], [out_vmem(size, bf16)], ())[0]

    part = embed_part(place, flat, 0, together, embed_table)
    own = summed(part)
    weights = loaded(part, gate_weight, up_weight, down_weight)
    state = start_of(own)
    sums_state, sums_hidden = [], []
    ticks = rounds + 3
    for tick in range(ticks):
        mine = [state]
        for s in (1, 2, 3):
            mine.append(along_x(state, s))
        theirs = [other_core(m) for m in mine]
        if tick == ticks - 1:
            far = (gate_weight, up_weight, down_weight)
            terms, base = call_last(place, mine, theirs, norm_gain, far, sums_hidden)
            sums_state.append(base)
            break
        send, keep, *pooled = call_mlp(place, mine, theirs, norm_gain, weights, tick >= 3)
        if tick >= 3:
            sums_hidden.append(pooled[0])
            sums_state.append(pooled[1])
        own, *out = local(
            halves_kernel, [], [keep, other_core(send)],
            [out_vmem(size, f32)] + [out_vmem(size, bf16)] * 3, (),
        )
        arrived = []
        for s in (2, 1, 3):
            arrived.append(along_x(out[s - 1], s))
        if tick + 1 < rounds:
            part = embed_part(place, flat, (tick + 1) * together, together, embed_table)
        if tick + 1 < rounds:
            fresh = start_of(summed(part))
        total = local(total_kernel, [place], [own, state, *arrived], out_vmem(size, bf16), ())
        ahead, kernel = [onward(total, 0), onward(total, 1)], join_kernel
        if tick + 1 < rounds:
            ahead, kernel = [*ahead, fresh], join_fresh_kernel
        state = local(kernel, [place], ahead, out_vmem(size, bf16), ())
    owners, members, final_gain, terms = lax.optimization_barrier(
        (owners, members, final_gain, terms)
    )

    groups = [[(g ^ ((m // 2) % 2)) * 16 + m for m in range(16)] for g in range(2)]
    pieces = lax.all_to_all(
        terms, ("dp", "mp"), 0, 0, tiled=True, axis_index_groups=groups
    )
    base = jnp.concatenate(sums_state, axis=0)
    pooled = jnp.sum(pieces, axis=0) + jnp.where(y == 0, base[:, :256], base[:, 256:])
    gain_here = lax.dynamic_slice_in_dim(final_gain, mp * 256, 256)
    value = (pooled * gain_here[None, :]).astype(bf16)
    everyone = lax.all_to_all(
        jnp.broadcast_to(value, (32, *value.shape)), ("dp", "mp"), 0, 0, tiled=True
    ).reshape(2, 16, *value.shape)

    prompts = owners.shape[0]
    here = prompts // 2
    slots = dp * here + jnp.arange(here, dtype=jnp.int32)
    match = (owners[None, :] == slots[:, None]).astype(jnp.int32)
    hit = match[:, :, None] * members.reshape(prompts, GROUP)[None]
    chosen = jnp.sum(hit, axis=1).reshape(here * GROUP, 1)
    chosen = jnp.pad(chosen, ((0, 128 - here * GROUP), (0, 0)), constant_values=-1)
    tile = head_part(
        jnp.reshape(mp, (1,)).astype(jnp.int32), chosen, everyone, final_gain[None], head_weight
    )
    rows = GROUP // 4
    got = lax.all_to_all(
        jnp.broadcast_to(tile, (16, GROUP, 128)), "mp", 0, 0, tiled=True
    )
    skew = jnp.sum(got, axis=0)
    options = jnp.stack([along_sections(skew, (s + 1) % 4) for s in range(3)] + [skew])
    skew = lax.dynamic_index_in_dim(options, section, 0, keepdims=False)
    skew = lax.dynamic_slice_in_dim(skew, section * rows, rows, 0)
    skew = jnp.stack([skew[:, p * GROUP : (p + 1) * GROUP] for p in range(here)])
    return jax.nn.sigmoid(skew)


def solution(mesh):
    placed = (
        P("dp", None),
        P(),
        P(),
        P("mp", "section"),
        P("section", None),
        P("section", None, "mp"),
        P("section", None, "mp"),
        P("section", None, "mp"),
        P(),
        P(None, "mp"),
    )
    return jax.shard_map(
        per_device, mesh=mesh, in_specs=placed, out_specs=P("dp", "section", None),
        check_vma=False,
    )
```

```python
import functools

import jax
import jax.numpy as jnp
from jax import lax
from jax.experimental import pallas as pl
from jax.experimental.pallas import tpu as pltpu
from jax.sharding import PartitionSpec as P


GROUP = 8
BLOCKS = 2
HALVES = 2
AXES = ("dp", "section", "mp")

norm_eps = 1e-05
final_eps = 1e-06
bf16 = jnp.bfloat16
f32 = jnp.float32


def moved(value, target):
    pairs = []
    for dp in range(2):
        for z in range(4):
            for x in range(4):
                for y in range(2):
                    for c in range(2):
                        to = target(dp, z, x, y, c)
                        if to is not None:
                            d, s, a, b, e = to
                            pairs.append(
                                (dp * 64 + z * 16 + x * 4 + y * 2 + c, d * 64 + s * 16 + a * 4 + b * 2 + e)
                            )
    return lax.ppermute(value, AXES, pairs)


def along_x(value, shift):
    return moved(value, lambda d, z, x, y, c: (d, z, (x + shift) % 4, y, c))


def other_core(value):
    return moved(value, lambda d, z, x, y, c: (d, z, x, y, 1 - c))


def other_dp(value):
    return moved(value, lambda d, z, x, y, c: (1 - d, z, x, y, c))


def other_y(value):
    return moved(value, lambda d, z, x, y, c: (1 - d, z, x, 1 - y, c))


def along_sections(value, shift):
    return moved(value, lambda d, z, x, y, c: (d, (z + shift) % 4, x, y, c))


def onward(value, flip):
    return moved(value, lambda d, z, x, y, c: (d ^ flip, (z + 1) % 4, x, y ^ flip, c))


def nt_dot(a, b):
    return lax.dot_general(a, b, (((1,), (1,)), ((), ())), preferred_element_type=f32)


def embed_kernel(width, first, place, ids_ref, table_ref, out, held, sems):
    rows = out.shape[0]
    ids = ids_ref[first : first + rows, :]
    steps = table_ref.shape[1] // width

    def copy(step):
        cols = pl.ds(pl.multiple_of(step * width, width), width)
        return pltpu.make_async_copy(table_ref.at[:, cols], held.at[:, cols], sems.at[step])

    def begin(step, carry):
        copy(step).start()
        return carry

    lax.fori_loop(0, steps, begin, 0)

    def one(step, acc):
        copy(step).wait()
        start = pl.multiple_of(step * width, width)
        hot = lax.broadcasted_iota(jnp.int32, (rows, width), 1) == ids - start
        return acc + nt_dot(hot.astype(f32).astype(bf16), held[:, pl.ds(start, width)])

    acc = lax.fori_loop(0, steps, one, jnp.zeros((rows, table_ref.shape[0]), f32))
    out[...] = acc.astype(bf16)


def cost(products):
    return pl.CostEstimate(flops=2 * products, bytes_accessed=0, transcendentals=0)


def in_hbm(value):
    return pltpu.with_memory_space_constraint(value, pltpu.HBM)


def in_vmem(value):
    return pltpu.with_memory_space_constraint(value, pltpu.VMEM)


VMEM_SPEC = pl.BlockSpec(memory_space=pltpu.VMEM)
HBM_SPEC = pl.BlockSpec(memory_space=pltpu.HBM)
SMEM_SPEC = pl.BlockSpec(memory_space=pltpu.SMEM)


def embed_part(place, ids, first, rows, table):
    width = 1024
    return pl.pallas_call(
        functools.partial(embed_kernel, width, first),
        in_specs=[SMEM_SPEC, VMEM_SPEC, HBM_SPEC],
        out_specs=VMEM_SPEC,
        out_shape=pltpu.VMEM((rows, table.shape[0]), bf16),
        scratch_shapes=[
            pltpu.VMEM(table.shape, bf16),
            pltpu.SemaphoreType.DMA((table.shape[1] // width,)),
        ],
        compiler_params=pltpu.CompilerParams(vmem_limit_bytes=14 * 1024 * 1024),
        cost_estimate=cost(rows * table.size),
        name="embed",
    )(place, in_vmem(ids), in_hbm(table))


def load_kernel(count, after, *refs):
    sources, places, sems = refs[:count], refs[count : 2 * count], refs[-1]
    copies = []
    for i, (source, place) in enumerate(zip(sources, places)):
        rows = source.shape[1] // 4
        for k in range(4):
            where = (0, pl.ds(k * rows, rows))
            copies.append(
                pltpu.make_async_copy(source.at[where], place.at[where], sems.at[4 * i + k])
            )
    for copy in copies:
        copy.start()
    for copy in copies:
        copy.wait()


def loaded(after, *arrays):
    count = len(arrays)
    return pl.pallas_call(
        functools.partial(load_kernel, count),
        in_specs=[VMEM_SPEC] + [HBM_SPEC] * count,
        out_specs=[VMEM_SPEC] * count,
        out_shape=[pltpu.VMEM(a.shape, a.dtype) for a in arrays],
        scratch_shapes=[pltpu.SemaphoreType.DMA((4 * count,))],
        compiler_params=pltpu.CompilerParams(vmem_limit_bytes=1024 * 1024),
        name="load",
    )(in_vmem(after), *[in_hbm(a) for a in arrays])


def prepare(x, c, chunks, gain_ref, scaled_ref, inverse_ref):
    count = chunks[0].shape[0]
    for half in range(HALVES):
        prepare_half(
            x, c, chunks[8 * half : 8 * half + 8], gain_ref,
            scaled_ref.at[half * count : (half + 1) * count, :],
            inverse_ref.at[half * count : (half + 1) * count, :],
        )


def prepare_half(x, c, chunks, gain_ref, scaled_ref, inverse_ref):
    def one(step, carry):
        rows = pl.ds(pl.multiple_of(step * 32, 32), 32)
        squares = None
        for shift in range(4):
            base = lax.rem(x + 4 - shift, 4) * 1024
            for ref, core in ((chunks[shift], c), (chunks[4 + shift], 1 - c)):
                for y in range(2):
                    block = ref[rows, y * 256 : (y + 1) * 256].astype(f32)
                    off = pl.multiple_of(base + y * 512 + core * 256, 256)
                    scaled_ref[rows, pl.ds(off, 256)] = (
                        block * gain_ref[:, pl.ds(off, 256)]
                    ).astype(bf16)
                    part = block[:, :128] * block[:, :128] + block[:, 128:] * block[:, 128:]
                    squares = part if squares is None else squares + part
        total = jnp.sum(squares, axis=1, keepdims=True)
        inverse_ref[rows, :] = jnp.broadcast_to(lax.rsqrt(total / 4096 + norm_eps), (32, 128))
        return carry

    lax.fori_loop(0, chunks[0].shape[0] // 32, one, 0)


def hidden_units(scaled, wg, wu, inverse_ref, gate_ref, up_ref, wait=None):
    def one(k, carry):
        if wait is not None:
            wait(0, k)
            wait(1, k)
        cols = pl.ds(pl.multiple_of(k * 1024, 1024), 1024)
        part = scaled[:, cols]
        gate = jnp.dot(part, wg[0, cols, :], preferred_element_type=f32)
        up = jnp.dot(part, wu[0, cols, :], preferred_element_type=f32)
        gate_ref[...] = jnp.where(k == 0, gate, gate_ref[...] + gate)
        up_ref[...] = jnp.where(k == 0, up, up_ref[...] + up)
        return carry

    lax.fori_loop(0, 4, one, 0)
    inverse = inverse_ref[:, :1]
    gate = gate_ref[...] * inverse
    return gate / (1.0 + jnp.exp(-gate)) * (up_ref[...] * inverse)


def mean_tokens(value):
    rows, cols = value.shape
    return jnp.sum(value.reshape(rows // 32, 32, cols), axis=1) * (1.0 / 32)


def base_means(chunks):
    return jnp.concatenate(
        [mean_tokens(chunks[8 * half][...].astype(f32)) for half in range(HALVES)], axis=0
    )


def mlp_kernel(pool, place, *refs):
    count = 8 * HALVES
    chunks, (gain, wg, wu, wd) = refs[:count], refs[count : count + 4]
    outs = refs[count + 4 : -4]
    send, keep = outs[:HALVES], outs[HALVES : 2 * HALVES]
    scaled, inverse, gate, up = refs[-4:]
    x, c = place[0], place[1]
    prepare(x, c, chunks, gain, scaled, inverse)
    hidden = hidden_units(scaled, wg, wu, inverse, gate, up)
    if pool:
        outs[-2][...] = mean_tokens(hidden)
        outs[-1][...] = base_means(chunks)
    rounded = hidden.astype(bf16)
    first = c == 0
    rows_half = chunks[0].shape[0]

    def one(s, carry):
        rows = pl.multiple_of(lax.rem(x + s, 4) * 1024, 1024)
        term = nt_dot(rounded, wd[0, pl.ds(rows, 1024), :])
        for y in range(2):
            a = term[:, y * 512 : y * 512 + 256]
            b = term[:, y * 512 + 256 : y * 512 + 512]
            cols = slice(y * 256, (y + 1) * 256)
            mine = jnp.where(first, a, b).astype(bf16)
            other = jnp.where(first, b, a).astype(bf16)
            for half in range(HALVES):
                part = slice(half * rows_half, (half + 1) * rows_half)
                keep[half][s, :, cols] = mine[part]
                send[half][s, :, cols] = other[part]
        return carry

    lax.fori_loop(0, 4, one, 0)


def last_kernel(count, place, *refs):
    first = 8 * HALVES
    chunks, gain, before = refs[:first], refs[first], refs[first + 1 : first + 1 + count]
    far, (out, base) = refs[first + 1 + count : first + 4 + count], refs[-10:-8]
    held, sems = refs[-8:-5], refs[-5]
    scaled, inverse, gate, up = refs[-4:]

    def copy(kind, k):
        rows = pl.ds(pl.multiple_of(k * 1024, 1024), 1024)
        return pltpu.make_async_copy(
            far[kind].at[0, rows, :], held[kind].at[0, rows, :], sems.at[kind * 4 + k]
        )

    def begin(k, carry):
        copy(0, k).start()
        copy(1, k).start()
        return carry

    def begin_down(k, carry):
        copy(2, k).start()
        return carry

    lax.fori_loop(0, 4, begin, 0)
    lax.fori_loop(0, 4, begin_down, 0)
    prepare(place[0], place[1], chunks, gain, scaled, inverse)
    hidden = hidden_units(
        scaled, held[0], held[1], inverse, gate, up, lambda kind, k: copy(kind, k).wait()
    )
    base[...] = base_means(chunks)
    every = jnp.concatenate([ref[...] for ref in before] + [mean_tokens(hidden)], axis=0)
    high = every.astype(bf16)
    low = (every - high.astype(f32)).astype(bf16)
    rows = every.shape[0]
    stacked = jnp.concatenate([high, low], axis=0)

    def one(k, carry):
        copy(2, k).wait()
        term = nt_dot(stacked, held[2][0, pl.ds(pl.multiple_of(k * 1024, 1024), 1024), :])
        term = term[:rows] + term[rows:]
        for m in range(4):
            out[4 * k + m] = term[:, m * 256 : (m + 1) * 256]
        return carry

    lax.fori_loop(0, 4, one, 0)


def gathered_kernel(own, a, b, d, out):
    out[...] = (
        own[...].astype(f32) + a[...].astype(f32) + (b[...].astype(f32) + d[...].astype(f32))
    ).astype(bf16)


def by_y(flag, own, peer):
    first = flag[2] == 0
    low, high = own[...].astype(f32), peer[...].astype(f32)
    return jnp.concatenate(
        [jnp.where(first, low, high), jnp.where(first, high, low)], axis=1
    )


def fresh_kernel(flag, own, peer, *out):
    whole = by_y(flag, own, peer).astype(bf16)
    rows = out[0].shape[0]
    for i, ref in enumerate(out):
        ref[...] = whole[i * rows : (i + 1) * rows]


def halves_kernel(keep, got, own, *out):
    own[...] = keep[0].astype(f32) + got[0].astype(f32)
    for s in range(1, 4):
        out[s - 1][...] = (keep[s].astype(f32) + got[s].astype(f32)).astype(bf16)


def total_kernel(flag, own, state, a, b, d, out):
    base = jnp.where(flag[2] == 0, state[...].astype(f32), 0.0)
    out[...] = (
        own[...] + base + (a[...].astype(f32) + b[...].astype(f32) + d[...].astype(f32))
    ).astype(bf16)


def join_kernel(flag, a, b, out):
    out[...] = (a[...].astype(f32) + b[...].astype(f32)).astype(bf16)


def join_fresh_kernel(flag, a, b, fresh, out):
    joined = (a[...].astype(f32) + b[...].astype(f32)).astype(bf16)
    out[...] = jnp.where(flag[3] == 0, fresh[...], joined)


def local(kernel, scalars, values, outs, scratch=(), limit=4, far=()):
    single = not isinstance(outs, list)
    return pl.pallas_call(
        kernel,
        in_specs=[SMEM_SPEC] * len(scalars) + [VMEM_SPEC] * len(values) + [HBM_SPEC] * len(far),
        out_specs=VMEM_SPEC if single else [VMEM_SPEC] * len(outs),
        out_shape=outs,
        scratch_shapes=list(scratch),
        compiler_params=pltpu.CompilerParams(vmem_limit_bytes=limit * 1024 * 1024),
    )(*scalars, *[in_vmem(v) for v in values], *[in_hbm(v) for v in far])


def out_vmem(shape, dtype):
    return pltpu.VMEM(shape, dtype)


def mlp_scratch(tokens):
    return [
        pltpu.VMEM((tokens, 4096), bf16),
        pltpu.VMEM((tokens, 128), f32),
        pltpu.VMEM((tokens, 640), f32),
        pltpu.VMEM((tokens, 640), f32),
    ]


def call_mlp(place, chunks, gain, weights, pool):
    count = chunks[0].shape[0]
    tokens = count * HALVES
    outs = [out_vmem((4, count, 512), bf16)] * (2 * HALVES)
    if pool:
        outs += [out_vmem((tokens // 32, 640), f32), out_vmem((tokens // 32, 512), f32)]
    result = local(
        functools.partial(mlp_kernel, pool), [place], [*chunks, gain, *weights], outs,
        mlp_scratch(tokens), 16,
    )
    return result[:HALVES], result[HALVES : 2 * HALVES], result[2 * HALVES :]


def call_last(place, chunks, gain, far, before):
    tokens = chunks[0].shape[0] * HALVES
    rows = sum(b.shape[0] for b in before) + tokens // 32
    return local(
        functools.partial(last_kernel, len(before)), [place], [*chunks, gain, *before],
        [out_vmem((16, rows, 256), f32), out_vmem((tokens // 32, 512), f32)],
        [pltpu.VMEM((1, 4096, 640), bf16)] * 3
        + [pltpu.SemaphoreType.DMA((12,))]
        + mlp_scratch(tokens),
        28, far,
    )


def head_kernel(place, chosen_ref, all_ref, gain_ref, head_ref, out_ref):
    total = squares = None
    for m in range(16):
        cols = slice(m * 256, (m + 1) * 256)
        side = (m // 2) % 2
        v = jnp.concatenate([all_ref[side, m], all_ref[1 - side, m]], axis=0)
        now = jnp.dot(v, head_ref[cols, :], preferred_element_type=f32)
        total = now if total is None else total + now
        plain = v.astype(f32) / gain_ref[:, cols]
        plain = plain * plain
        plain = plain[:, :128] + plain[:, 128:]
        squares = plain if squares is None else squares + plain
    factor = lax.rsqrt(jnp.sum(squares, axis=1, keepdims=True) / 4096 + final_eps)
    here = place[0]
    side = lax.rem(here // 2, 2)
    mine = jnp.concatenate([all_ref[side, here], all_ref[1 - side, here]], axis=0)
    mine = mine.astype(f32) * factor
    scores = lax.dot_general(
        total * factor, mine, (((1,), (1,)), ((), ())),
        precision=lax.Precision.HIGHEST, preferred_element_type=f32,
    )
    skew = scores - scores.T
    chosen = chosen_ref[...]
    count = skew.shape[0]
    hot = (lax.broadcasted_iota(jnp.int32, (chosen.shape[0], count), 1) == chosen).astype(f32)
    half = out_ref.shape[0]
    rows = jnp.dot(hot[: 2 * half], skew, precision=lax.Precision.HIGHEST, preferred_element_type=f32)
    tile = lax.dot_general(
        rows, hot, (((1,), (1,)), ((), ())),
        precision=lax.Precision.HIGHEST, preferred_element_type=f32,
    )
    lane = lax.broadcasted_iota(jnp.int32, out_ref.shape, 1)
    out_ref[...] = jnp.where(lane < half, tile[:half], tile[half:])


def head_part(place, chosen, everyone, gain, head):
    vmem = pl.BlockSpec(memory_space=pltpu.VMEM)
    return pl.pallas_call(
        head_kernel,
        in_specs=[pl.BlockSpec(memory_space=pltpu.SMEM)] + [vmem] * 4,
        out_specs=vmem,
        out_shape=jax.ShapeDtypeStruct((GROUP, chosen.shape[0]), f32),
        name="head",
    )(place, chosen, everyone, gain, head)


def per_device(
    token_ids, members, owners, embed_table, norm_gain, gate_weight, up_weight, down_weight,
    final_gain, head_weight,
):
    section = lax.axis_index("section")
    mp = lax.axis_index("mp")
    dp = lax.axis_index("dp")
    x, y, c = mp // 4, (mp // 2) % 2, mp % 2
    place = jnp.stack([x, c, y, section]).astype(jnp.int32)
    ids = jnp.where(y == 0, token_ids, other_dp(token_ids))
    flat = ids.reshape(-1, 1) - section * embed_table.shape[1]
    together = flat.shape[0] // BLOCKS
    size = (together // HALVES, 512)

    def summed(part):
        pieces = []
        for z in (1, 3, 2):
            pieces.append(along_sections(part, z))
        return local(gathered_kernel, [], [part, *pieces], out_vmem(part.shape, bf16), ())

    def start_of(own):
        return local(
            fresh_kernel, [place], [own, other_y(own)], [out_vmem(size, bf16)] * HALVES, ()
        )

    part = embed_part(place, flat, 0, together, embed_table)
    own = summed(part)
    weights = loaded(part, gate_weight, up_weight, down_weight)
    states = start_of(own)
    sums_state, sums_hidden = [], []
    ticks = BLOCKS + 3
    for tick in range(ticks):
        chunks = []
        for state in states:
            mine = [state] + [along_x(state, s) for s in (1, 2, 3)]
            chunks += [*mine, *[other_core(m) for m in mine]]
        if tick == ticks - 1:
            far = (gate_weight, up_weight, down_weight)
            terms, base = call_last(place, chunks, norm_gain, far, sums_hidden)
            sums_state.append(base)
            break
        send, keep, pooled = call_mlp(place, chunks, norm_gain, weights, tick >= 3)
        if tick >= 3:
            sums_hidden.append(pooled[0])
            sums_state.append(pooled[1])
        moving = []
        for half in range(HALVES):
            own, *out = local(
                halves_kernel, [], [keep[half], other_core(send[half])],
                [out_vmem(size, f32)] + [out_vmem(size, bf16)] * 3, (),
            )
            arrived = []
            for s in (1, 2, 3):
                arrived.append(along_x(out[s - 1], s))
            moving.append((own, arrived))
        if tick + 1 < BLOCKS:
            part = embed_part(place, flat, (tick + 1) * together, together, embed_table)
        if tick + 1 < BLOCKS:
            fresh = start_of(summed(part))
        following = []
        for half, (own, arrived) in enumerate(moving):
            total = local(
                total_kernel, [place], [own, states[half], *arrived], out_vmem(size, bf16), (),
            )
            ahead, kernel = [onward(total, 0), onward(total, 1)], join_kernel
            if tick + 1 < BLOCKS:
                ahead, kernel = [*ahead, fresh[half]], join_fresh_kernel
            following.append(local(kernel, [place], ahead, out_vmem(size, bf16), ()))
        states = following
    owners, members, final_gain, terms = lax.optimization_barrier(
        (owners, members, final_gain, terms)
    )

    groups = [[(g ^ ((m // 2) % 2)) * 16 + m for m in range(16)] for g in range(2)]
    pieces = lax.all_to_all(
        terms, ("dp", "mp"), 0, 0, tiled=True, axis_index_groups=groups
    )
    base = jnp.concatenate(sums_state, axis=0)
    pooled = jnp.sum(pieces, axis=0) + jnp.where(y == 0, base[:, :256], base[:, 256:])
    gain_here = lax.dynamic_slice_in_dim(final_gain, mp * 256, 256)
    value = (pooled * gain_here[None, :]).astype(bf16)
    everyone = lax.all_to_all(
        jnp.broadcast_to(value, (32, *value.shape)), ("dp", "mp"), 0, 0, tiled=True
    ).reshape(2, 16, *value.shape)

    prompts = owners.shape[0]
    here = prompts // 2
    slots = dp * here + jnp.arange(here, dtype=jnp.int32)
    match = (owners[None, :] == slots[:, None]).astype(jnp.int32)
    hit = match[:, :, None] * members.reshape(prompts, GROUP)[None]
    chosen = jnp.sum(hit, axis=1).reshape(here * GROUP, 1)
    chosen = jnp.pad(chosen, ((0, 128 - here * GROUP), (0, 0)), constant_values=-1)
    tile = head_part(
        jnp.reshape(mp, (1,)).astype(jnp.int32), chosen, everyone, final_gain[None], head_weight
    )
    rows = GROUP // 4
    got = lax.all_to_all(
        jnp.broadcast_to(tile, (16, GROUP, 128)), "mp", 0, 0, tiled=True
    )
    skew = jnp.sum(got, axis=0)
    options = jnp.stack([along_sections(skew, (s + 1) % 4) for s in range(3)] + [skew])
    skew = lax.dynamic_index_in_dim(options, section, 0, keepdims=False)
    skew = lax.dynamic_slice_in_dim(skew, section * rows, rows, 0)
    skew = jnp.stack([skew[:, p * GROUP : (p + 1) * GROUP] for p in range(here)])
    return jax.nn.sigmoid(skew)


def solution(mesh):
    placed = (
        P("dp", None),
        P(),
        P(),
        P("mp", "section"),
        P("section", None),
        P("section", None, "mp"),
        P("section", None, "mp"),
        P("section", None, "mp"),
        P(),
        P(None, "mp"),
    )
    return jax.shard_map(
        per_device, mesh=mesh, in_specs=placed, out_specs=P("dp", "section", None),
        check_vma=False,
    )
```

```python
import functools

import jax
import jax.numpy as jnp
from jax import lax
from jax.experimental import pallas as pl
from jax.experimental.pallas import tpu as pltpu
from jax.sharding import PartitionSpec as P


GROUP = 8
BLOCKS = 2
HALVES = 2
AXES = ("dp", "section", "mp")

norm_eps = 1e-05
final_eps = 1e-06
bf16 = jnp.bfloat16
f32 = jnp.float32


def moved(value, target):
    pairs = []
    for dp in range(2):
        for z in range(4):
            for x in range(4):
                for y in range(2):
                    for c in range(2):
                        to = target(dp, z, x, y, c)
                        if to is not None:
                            d, s, a, b, e = to
                            pairs.append(
                                (dp * 64 + z * 16 + x * 4 + y * 2 + c, d * 64 + s * 16 + a * 4 + b * 2 + e)
                            )
    return lax.ppermute(value, AXES, pairs)


def along_x(value, shift):
    return moved(value, lambda d, z, x, y, c: (d, z, (x + shift) % 4, y, c))


def other_core(value):
    return moved(value, lambda d, z, x, y, c: (d, z, x, y, 1 - c))


def other_dp(value):
    return moved(value, lambda d, z, x, y, c: (1 - d, z, x, y, c))


def other_y(value):
    return moved(value, lambda d, z, x, y, c: (1 - d, z, x, 1 - y, c))


def along_sections(value, shift):
    return moved(value, lambda d, z, x, y, c: (d, (z + shift) % 4, x, y, c))


def onward(value, flip):
    return moved(value, lambda d, z, x, y, c: (d ^ flip, (z + 1) % 4, x, y ^ flip, c))


def nt_dot(a, b):
    return lax.dot_general(a, b, (((1,), (1,)), ((), ())), preferred_element_type=f32)


def embed_kernel(width, first, place, ids_ref, table_ref, out, held, sems):
    rows = out.shape[0]
    ids = ids_ref[:, first : first + rows]
    steps = table_ref.shape[1] // width

    def copy(step):
        cols = pl.ds(pl.multiple_of(step * width, width), width)
        return pltpu.make_async_copy(table_ref.at[:, cols], held.at[:, cols], sems.at[step])

    def begin(step, carry):
        copy(step).start()
        return carry

    lax.fori_loop(0, steps, begin, 0)

    def one(step, acc):
        copy(step).wait()
        start = pl.multiple_of(step * width, width)
        hot = lax.broadcasted_iota(jnp.int32, (width, rows), 0) == ids - start
        return acc + jnp.dot(
            held[:, pl.ds(start, width)], hot.astype(f32).astype(bf16), preferred_element_type=f32
        )

    acc = lax.fori_loop(0, steps, one, jnp.zeros((table_ref.shape[0], rows), f32))
    out[...] = acc.T.astype(bf16)


def cost(products):
    return pl.CostEstimate(flops=2 * products, bytes_accessed=0, transcendentals=0)


def in_hbm(value):
    return pltpu.with_memory_space_constraint(value, pltpu.HBM)


def in_vmem(value):
    return pltpu.with_memory_space_constraint(value, pltpu.VMEM)


VMEM_SPEC = pl.BlockSpec(memory_space=pltpu.VMEM)
HBM_SPEC = pl.BlockSpec(memory_space=pltpu.HBM)
SMEM_SPEC = pl.BlockSpec(memory_space=pltpu.SMEM)


def embed_part(place, ids, first, rows, table):
    width = 2048
    return pl.pallas_call(
        functools.partial(embed_kernel, width, first),
        in_specs=[SMEM_SPEC, VMEM_SPEC, HBM_SPEC],
        out_specs=VMEM_SPEC,
        out_shape=pltpu.VMEM((rows, table.shape[0]), bf16),
        scratch_shapes=[
            pltpu.VMEM(table.shape, bf16),
            pltpu.SemaphoreType.DMA((table.shape[1] // width,)),
        ],
        compiler_params=pltpu.CompilerParams(vmem_limit_bytes=20 * 1024 * 1024),
        cost_estimate=cost(rows * table.size),
        name="embed",
    )(place, in_vmem(ids), in_hbm(table))


def load_kernel(count, after, *refs):
    sources, places, sems = refs[:count], refs[count : 2 * count], refs[-1]
    copies = []
    for i, (source, place) in enumerate(zip(sources, places)):
        rows = source.shape[1] // 4
        for k in range(4):
            where = (0, pl.ds(k * rows, rows))
            copies.append(
                pltpu.make_async_copy(source.at[where], place.at[where], sems.at[4 * i + k])
            )
    for copy in copies:
        copy.start()
    for copy in copies:
        copy.wait()


def loaded(after, *arrays):
    count = len(arrays)
    return pl.pallas_call(
        functools.partial(load_kernel, count),
        in_specs=[VMEM_SPEC] + [HBM_SPEC] * count,
        out_specs=[VMEM_SPEC] * count,
        out_shape=[pltpu.VMEM(a.shape, a.dtype) for a in arrays],
        scratch_shapes=[pltpu.SemaphoreType.DMA((4 * count,))],
        compiler_params=pltpu.CompilerParams(vmem_limit_bytes=1024 * 1024),
        name="load",
    )(in_vmem(after), *[in_hbm(a) for a in arrays])


def prepare(x, c, chunks, gain_ref, scaled_ref, inverse_ref):
    count = chunks[0].shape[0]
    for half in range(HALVES):
        prepare_half(
            x, c, chunks[8 * half : 8 * half + 8], gain_ref,
            scaled_ref.at[half * count : (half + 1) * count, :],
            inverse_ref.at[half * count : (half + 1) * count, :],
        )


def prepare_half(x, c, chunks, gain_ref, scaled_ref, inverse_ref):
    def one(step, carry):
        rows = pl.ds(pl.multiple_of(step * 32, 32), 32)
        squares = None
        for shift in range(4):
            base = lax.rem(x + 4 - shift, 4) * 1024
            for ref, core in ((chunks[shift], c), (chunks[4 + shift], 1 - c)):
                for y in range(2):
                    block = ref[rows, y * 256 : (y + 1) * 256].astype(f32)
                    off = pl.multiple_of(base + y * 512 + core * 256, 256)
                    scaled_ref[rows, pl.ds(off, 256)] = (
                        block * gain_ref[:, pl.ds(off, 256)]
                    ).astype(bf16)
                    part = block[:, :128] * block[:, :128] + block[:, 128:] * block[:, 128:]
                    squares = part if squares is None else squares + part
        total = jnp.sum(squares, axis=1, keepdims=True)
        inverse_ref[rows, :] = jnp.broadcast_to(lax.rsqrt(total / 4096 + norm_eps), (32, 128))
        return carry

    lax.fori_loop(0, chunks[0].shape[0] // 32, one, 0)


def activated(gate, up, inverse):
    gate = gate * inverse
    return gate / (1.0 + jnp.exp(-gate)) * (up * inverse)


def hidden_units(scaled, wg, wu, inverse_ref, gate_ref, up_ref, wait):
    def one(k, carry):
        wait(0, k)
        wait(1, k)
        cols = pl.ds(pl.multiple_of(k * 1024, 1024), 1024)
        part = scaled[:, cols]
        gate = jnp.dot(part, wg[0, cols, :], preferred_element_type=f32)
        up = jnp.dot(part, wu[0, cols, :], preferred_element_type=f32)
        gate_ref[...] = jnp.where(k == 0, gate, gate_ref[...] + gate)
        up_ref[...] = jnp.where(k == 0, up, up_ref[...] + up)
        return carry

    lax.fori_loop(0, 4, one, 0)
    return activated(gate_ref[...], up_ref[...], inverse_ref[:, :1])


def mean_tokens(value):
    rows, cols = value.shape
    return jnp.sum(value.reshape(rows // 32, 32, cols), axis=1) * (1.0 / 32)


def base_means(chunks):
    return jnp.concatenate(
        [mean_tokens(chunks[8 * half][...].astype(f32)) for half in range(HALVES)], axis=0
    )


def mlp_kernel(pool, place, *refs):
    count = 8 * HALVES
    chunks, (gain, wg, wu, wd) = refs[:count], refs[count : count + 4]
    outs = refs[count + 4 : -2]
    send, keep = outs[:HALVES], outs[HALVES : 2 * HALVES]
    scaled, inverse = refs[-2:]
    x, c = place[0], place[1]
    prepare(x, c, chunks, gain, scaled, inverse)
    gate = jnp.dot(scaled[...], wg[0], preferred_element_type=f32)
    up = jnp.dot(scaled[...], wu[0], preferred_element_type=f32)
    hidden = activated(gate, up, inverse[:, :1])
    if pool:
        outs[-2][...] = mean_tokens(hidden)
        outs[-1][...] = base_means(chunks)
    rounded = hidden.astype(bf16)
    first = c == 0
    rows_half = chunks[0].shape[0]

    def one(s, carry):
        rows = pl.multiple_of(lax.rem(x + s, 4) * 1024, 1024)
        term = nt_dot(rounded, wd[0, pl.ds(rows, 1024), :])
        for y in range(2):
            a = term[:, y * 512 : y * 512 + 256]
            b = term[:, y * 512 + 256 : y * 512 + 512]
            cols = slice(y * 256, (y + 1) * 256)
            mine = jnp.where(first, a, b).astype(bf16)
            other = jnp.where(first, b, a).astype(bf16)
            for half in range(HALVES):
                part = slice(half * rows_half, (half + 1) * rows_half)
                keep[half][s, :, cols] = mine[part]
                send[half][s, :, cols] = other[part]
        return carry

    lax.fori_loop(0, 4, one, 0)


def last_kernel(count, place, *refs):
    first = 8 * HALVES
    chunks, gain, before = refs[:first], refs[first], refs[first + 1 : first + 1 + count]
    far, (out, base) = refs[first + 1 + count : first + 4 + count], refs[-10:-8]
    held, sems = refs[-8:-5], refs[-5]
    scaled, inverse, gate, up = refs[-4:]

    def copy(kind, k):
        rows = pl.ds(pl.multiple_of(k * 1024, 1024), 1024)
        return pltpu.make_async_copy(
            far[kind].at[0, rows, :], held[kind].at[0, rows, :], sems.at[kind * 4 + k]
        )

    def begin(k, carry):
        copy(0, k).start()
        copy(1, k).start()
        return carry

    def begin_down(k, carry):
        copy(2, k).start()
        return carry

    lax.fori_loop(0, 4, begin, 0)
    lax.fori_loop(0, 4, begin_down, 0)
    prepare(place[0], place[1], chunks, gain, scaled, inverse)
    hidden = hidden_units(
        scaled, held[0], held[1], inverse, gate, up, lambda kind, k: copy(kind, k).wait()
    )
    base[...] = base_means(chunks)
    every = jnp.concatenate([ref[...] for ref in before] + [mean_tokens(hidden)], axis=0)
    high = every.astype(bf16)
    low = (every - high.astype(f32)).astype(bf16)
    rows = every.shape[0]
    stacked = jnp.concatenate([high, low], axis=0)

    def one(k, carry):
        copy(2, k).wait()
        term = nt_dot(stacked, held[2][0, pl.ds(pl.multiple_of(k * 1024, 1024), 1024), :])
        term = term[:rows] + term[rows:]
        for m in range(4):
            out[4 * k + m] = term[:, m * 256 : (m + 1) * 256]
        return carry

    lax.fori_loop(0, 4, one, 0)


def gathered_kernel(own, a, b, d, out):
    out[...] = (
        own[...].astype(f32) + a[...].astype(f32) + (b[...].astype(f32) + d[...].astype(f32))
    ).astype(bf16)


def by_y(flag, own, peer):
    first = flag[2] == 0
    low, high = own[...].astype(f32), peer[...].astype(f32)
    return jnp.concatenate(
        [jnp.where(first, low, high), jnp.where(first, high, low)], axis=1
    )


def fresh_kernel(flag, own, peer, *out):
    whole = by_y(flag, own, peer).astype(bf16)
    rows = out[0].shape[0]
    for i, ref in enumerate(out):
        ref[...] = whole[i * rows : (i + 1) * rows]


def halves_kernel(keep, got, own, right, across, left):
    own[...] = keep[0].astype(f32) + got[0].astype(f32)
    right[...] = (keep[1].astype(f32) + got[1].astype(f32)).astype(bf16)
    across[...] = (keep[2].astype(f32) + got[2].astype(f32)).astype(bf16)
    left[...] = keep[3].astype(f32) + got[3].astype(f32)


def relay_kernel(left, passing, out):
    out[...] = (left[...] + passing[...].astype(f32)).astype(bf16)


def total_kernel(flag, own, state, a, b, out):
    base = jnp.where(flag[2] == 0, state[...].astype(f32), 0.0)
    out[...] = (own[...] + base + (a[...].astype(f32) + b[...].astype(f32))).astype(bf16)


def join_kernel(flag, a, b, out):
    out[...] = (a[...].astype(f32) + b[...].astype(f32)).astype(bf16)


def join_fresh_kernel(flag, a, b, fresh, out):
    joined = (a[...].astype(f32) + b[...].astype(f32)).astype(bf16)
    out[...] = jnp.where(flag[3] == 0, fresh[...], joined)


def local(kernel, scalars, values, outs, scratch=(), limit=4, far=()):
    single = not isinstance(outs, list)
    return pl.pallas_call(
        kernel,
        in_specs=[SMEM_SPEC] * len(scalars) + [VMEM_SPEC] * len(values) + [HBM_SPEC] * len(far),
        out_specs=VMEM_SPEC if single else [VMEM_SPEC] * len(outs),
        out_shape=outs,
        scratch_shapes=list(scratch),
        compiler_params=pltpu.CompilerParams(vmem_limit_bytes=limit * 1024 * 1024),
    )(*scalars, *[in_vmem(v) for v in values], *[in_hbm(v) for v in far])


def out_vmem(shape, dtype):
    return pltpu.VMEM(shape, dtype)


def mlp_scratch(tokens):
    return [
        pltpu.VMEM((tokens, 4096), bf16),
        pltpu.VMEM((tokens, 128), f32),
        pltpu.VMEM((tokens, 640), f32),
        pltpu.VMEM((tokens, 640), f32),
    ]


def call_mlp(place, chunks, gain, weights, pool):
    count = chunks[0].shape[0]
    tokens = count * HALVES
    outs = [out_vmem((4, count, 512), bf16)] * (2 * HALVES)
    if pool:
        outs += [out_vmem((tokens // 32, 640), f32), out_vmem((tokens // 32, 512), f32)]
    result = local(
        functools.partial(mlp_kernel, pool), [place], [*chunks, gain, *weights], outs,
        mlp_scratch(tokens)[:2], 16,
    )
    return result[:HALVES], result[HALVES : 2 * HALVES], result[2 * HALVES :]


def call_last(place, chunks, gain, far, before):
    tokens = chunks[0].shape[0] * HALVES
    rows = sum(b.shape[0] for b in before) + tokens // 32
    return local(
        functools.partial(last_kernel, len(before)), [place], [*chunks, gain, *before],
        [out_vmem((16, rows, 256), f32), out_vmem((tokens // 32, 512), f32)],
        [pltpu.VMEM((1, 4096, 640), bf16)] * 3
        + [pltpu.SemaphoreType.DMA((12,))]
        + mlp_scratch(tokens),
        28, far,
    )


def head_kernel(place, chosen_ref, all_ref, gain_ref, head_ref, out_ref):
    total = squares = None
    for m in range(16):
        cols = slice(m * 256, (m + 1) * 256)
        side = (m // 2) % 2
        v = jnp.concatenate([all_ref[side, m], all_ref[1 - side, m]], axis=0)
        now = jnp.dot(v, head_ref[cols, :], preferred_element_type=f32)
        total = now if total is None else total + now
        plain = v.astype(f32) / gain_ref[:, cols]
        plain = plain * plain
        plain = plain[:, :128] + plain[:, 128:]
        squares = plain if squares is None else squares + plain
    factor = lax.rsqrt(jnp.sum(squares, axis=1, keepdims=True) / 4096 + final_eps)
    here = place[0]
    side = lax.rem(here // 2, 2)
    mine = jnp.concatenate([all_ref[side, here], all_ref[1 - side, here]], axis=0)
    mine = mine.astype(f32) * factor
    scores = lax.dot_general(
        total * factor, mine, (((1,), (1,)), ((), ())),
        precision=lax.Precision.HIGHEST, preferred_element_type=f32,
    )
    skew = scores - scores.T
    chosen = chosen_ref[...]
    count = skew.shape[0]
    hot = (lax.broadcasted_iota(jnp.int32, (chosen.shape[0], count), 1) == chosen).astype(f32)
    half = out_ref.shape[0]
    rows = jnp.dot(hot[: 2 * half], skew, precision=lax.Precision.HIGHEST, preferred_element_type=f32)
    tile = lax.dot_general(
        rows, hot, (((1,), (1,)), ((), ())),
        precision=lax.Precision.HIGHEST, preferred_element_type=f32,
    )
    lane = lax.broadcasted_iota(jnp.int32, out_ref.shape, 1)
    out_ref[...] = jnp.where(lane < half, tile[:half], tile[half:])


def head_part(place, chosen, everyone, gain, head):
    vmem = pl.BlockSpec(memory_space=pltpu.VMEM)
    return pl.pallas_call(
        head_kernel,
        in_specs=[pl.BlockSpec(memory_space=pltpu.SMEM)] + [vmem] * 4,
        out_specs=vmem,
        out_shape=jax.ShapeDtypeStruct((GROUP, chosen.shape[0]), f32),
        name="head",
    )(place, chosen, everyone, gain, head)


def per_device(
    token_ids, members, owners, embed_table, norm_gain, gate_weight, up_weight, down_weight,
    final_gain, head_weight,
):
    section = lax.axis_index("section")
    mp = lax.axis_index("mp")
    dp = lax.axis_index("dp")
    x, y, c = mp // 4, (mp // 2) % 2, mp % 2
    place = jnp.stack([x, c, y, section]).astype(jnp.int32)
    ids = jnp.where(y == 0, token_ids, other_dp(token_ids))
    flat = ids.reshape(1, -1) - section * embed_table.shape[1]
    together = flat.shape[1] // BLOCKS
    size = (together // HALVES, 512)

    def summed(part):
        pieces = []
        for z in (1, 3, 2):
            pieces.append(along_sections(part, z))
        return local(gathered_kernel, [], [part, *pieces], out_vmem(part.shape, bf16), ())

    def start_of(own):
        return local(
            fresh_kernel, [place], [own, other_y(own)], [out_vmem(size, bf16)] * HALVES, ()
        )

    part = embed_part(place, flat, 0, together, embed_table)
    own = summed(part)
    weights = loaded(part, gate_weight, up_weight, down_weight)
    states = start_of(own)
    sums_state, sums_hidden = [], []
    ticks = BLOCKS + 3
    for tick in range(ticks):
        chunks = []
        for state in states:
            near = along_x(state, 1)
            mine = [state, near, along_x(near, 1), along_x(state, 3)]
            chunks += [*mine, *[other_core(m) for m in mine]]
        if tick == ticks - 1:
            far = (gate_weight, up_weight, down_weight)
            terms, base = call_last(place, chunks, norm_gain, far, sums_hidden)
            sums_state.append(base)
            break
        send, keep, pooled = call_mlp(place, chunks, norm_gain, weights, tick >= 3)
        if tick >= 3:
            sums_hidden.append(pooled[0])
            sums_state.append(pooled[1])
        moving = []
        for half in range(HALVES):
            own, right, across, left = local(
                halves_kernel, [], [keep[half], other_core(send[half])],
                [out_vmem(size, t) for t in (f32, bf16, bf16, f32)], (),
            )
            passing = along_x(across, 3)
            arrived = [along_x(right, 1)]
            left = local(relay_kernel, [], [left, passing], out_vmem(size, bf16), ())
            arrived.append(along_x(left, 3))
            moving.append((own, arrived))
        if tick + 1 < BLOCKS:
            part = embed_part(place, flat, (tick + 1) * together, together, embed_table)
        if tick + 1 < BLOCKS:
            fresh = start_of(summed(part))
        following = []
        for half, (own, arrived) in enumerate(moving):
            total = local(
                total_kernel, [place], [own, states[half], *arrived], out_vmem(size, bf16), (),
            )
            ahead, kernel = [onward(total, 0), onward(total, 1)], join_kernel
            if tick + 1 < BLOCKS:
                ahead, kernel = [*ahead, fresh[half]], join_fresh_kernel
            following.append(local(kernel, [place], ahead, out_vmem(size, bf16), ()))
        states = following
    owners, members, final_gain, terms = lax.optimization_barrier(
        (owners, members, final_gain, terms)
    )

    groups = [[(g ^ ((m // 2) % 2)) * 16 + m for m in range(16)] for g in range(2)]
    pieces = lax.all_to_all(
        terms, ("dp", "mp"), 0, 0, tiled=True, axis_index_groups=groups
    )
    base = jnp.concatenate(sums_state, axis=0)
    pooled = jnp.sum(pieces, axis=0) + jnp.where(y == 0, base[:, :256], base[:, 256:])
    gain_here = lax.dynamic_slice_in_dim(final_gain, mp * 256, 256)
    value = (pooled * gain_here[None, :]).astype(bf16)
    everyone = lax.all_to_all(
        jnp.broadcast_to(value, (32, *value.shape)), ("dp", "mp"), 0, 0, tiled=True
    ).reshape(2, 16, *value.shape)

    prompts = owners.shape[0]
    here = prompts // 2
    slots = dp * here + jnp.arange(here, dtype=jnp.int32)
    match = (owners[None, :] == slots[:, None]).astype(jnp.int32)
    hit = match[:, :, None] * members.reshape(prompts, GROUP)[None]
    chosen = jnp.sum(hit, axis=1).reshape(here * GROUP, 1)
    chosen = jnp.pad(chosen, ((0, 128 - here * GROUP), (0, 0)), constant_values=-1)
    tile = head_part(
        jnp.reshape(mp, (1,)).astype(jnp.int32), chosen, everyone, final_gain[None], head_weight
    )
    rows = GROUP // 4
    got = lax.all_to_all(
        jnp.broadcast_to(tile, (16, GROUP, 128)), "mp", 0, 0, tiled=True
    )
    skew = jnp.sum(got, axis=0)
    options = jnp.stack([along_sections(skew, (s + 1) % 4) for s in range(3)] + [skew])
    skew = lax.dynamic_index_in_dim(options, section, 0, keepdims=False)
    skew = lax.dynamic_slice_in_dim(skew, section * rows, rows, 0)
    skew = jnp.stack([skew[:, p * GROUP : (p + 1) * GROUP] for p in range(here)])
    return jax.nn.sigmoid(skew)


def solution(mesh):
    placed = (
        P("dp", None),
        P(),
        P(),
        P("mp", "section"),
        P("section", None),
        P("section", None, "mp"),
        P("section", None, "mp"),
        P("section", None, "mp"),
        P(),
        P(None, "mp"),
    )
    return jax.shard_map(
        per_device, mesh=mesh, in_specs=placed, out_specs=P("dp", "section", None),
        check_vma=False,
    )
```

```python
import functools

import jax
import jax.numpy as jnp
from jax import lax
from jax.experimental import pallas as pl
from jax.experimental.pallas import tpu as pltpu
from jax.sharding import PartitionSpec as P


GROUP = 8
BLOCKS = 2
HALVES = 2
AXES = ("dp", "section", "mp")

norm_eps = 1e-05
final_eps = 1e-06
bf16 = jnp.bfloat16
f32 = jnp.float32


def moved(value, target):
    pairs = []
    for dp in range(2):
        for z in range(4):
            for x in range(4):
                for y in range(2):
                    for c in range(2):
                        to = target(dp, z, x, y, c)
                        if to is not None:
                            d, s, a, b, e = to
                            pairs.append(
                                (dp * 64 + z * 16 + x * 4 + y * 2 + c, d * 64 + s * 16 + a * 4 + b * 2 + e)
                            )
    return lax.ppermute(value, AXES, pairs)


def along_x(value, shift):
    return moved(value, lambda d, z, x, y, c: (d, z, (x + shift) % 4, y, c))


def other_core(value):
    return moved(value, lambda d, z, x, y, c: (d, z, x, y, 1 - c))


def other_dp(value):
    return moved(value, lambda d, z, x, y, c: (1 - d, z, x, y, c))


def other_y(value):
    return moved(value, lambda d, z, x, y, c: (1 - d, z, x, 1 - y, c))


def along_sections(value, shift):
    return moved(value, lambda d, z, x, y, c: (d, (z + shift) % 4, x, y, c))


def onward(value, flip):
    return moved(value, lambda d, z, x, y, c: (d ^ flip, (z + 1) % 4, x, y ^ flip, c))


def nt_dot(a, b):
    return lax.dot_general(a, b, (((1,), (1,)), ((), ())), preferred_element_type=f32)


def embed_kernel(width, first, place, ids_ref, table_ref, out, held, sems):
    rows = out.shape[0]
    ids = ids_ref[:, first : first + rows]
    steps = table_ref.shape[1] // width

    def copy(step):
        cols = pl.ds(pl.multiple_of(step * width, width), width)
        return pltpu.make_async_copy(table_ref.at[:, cols], held.at[:, cols], sems.at[step])

    def begin(step, carry):
        copy(step).start()
        return carry

    lax.fori_loop(0, steps, begin, 0)

    def one(step, acc):
        copy(step).wait()
        start = pl.multiple_of(step * width, width)
        hot = lax.broadcasted_iota(jnp.int32, (width, rows), 0) == ids - start
        return acc + jnp.dot(
            held[:, pl.ds(start, width)], hot.astype(f32).astype(bf16), preferred_element_type=f32
        )

    acc = lax.fori_loop(0, steps, one, jnp.zeros((table_ref.shape[0], rows), f32))
    out[...] = acc.T.astype(bf16)


def cost(products):
    return pl.CostEstimate(flops=2 * products, bytes_accessed=0, transcendentals=0)


def in_hbm(value):
    return pltpu.with_memory_space_constraint(value, pltpu.HBM)


def in_vmem(value):
    return pltpu.with_memory_space_constraint(value, pltpu.VMEM)


VMEM_SPEC = pl.BlockSpec(memory_space=pltpu.VMEM)
HBM_SPEC = pl.BlockSpec(memory_space=pltpu.HBM)
SMEM_SPEC = pl.BlockSpec(memory_space=pltpu.SMEM)


def embed_part(place, ids, first, rows, table):
    width = 2048
    return pl.pallas_call(
        functools.partial(embed_kernel, width, first),
        in_specs=[SMEM_SPEC, VMEM_SPEC, HBM_SPEC],
        out_specs=VMEM_SPEC,
        out_shape=pltpu.VMEM((rows, table.shape[0]), bf16),
        scratch_shapes=[
            pltpu.VMEM(table.shape, bf16),
            pltpu.SemaphoreType.DMA((table.shape[1] // width,)),
        ],
        compiler_params=pltpu.CompilerParams(vmem_limit_bytes=20 * 1024 * 1024),
        cost_estimate=cost(rows * table.size),
        name="embed",
    )(place, in_vmem(ids), in_hbm(table))


def load_kernel(count, after, *refs):
    sources, places, sems = refs[:count], refs[count : 2 * count], refs[-1]
    copies = []
    for i, (source, place) in enumerate(zip(sources, places)):
        rows = source.shape[1] // 4
        for k in range(4):
            where = (0, pl.ds(k * rows, rows))
            copies.append(
                pltpu.make_async_copy(source.at[where], place.at[where], sems.at[4 * i + k])
            )
    for copy in copies:
        copy.start()
    for copy in copies:
        copy.wait()


def loaded(after, *arrays):
    count = len(arrays)
    return pl.pallas_call(
        functools.partial(load_kernel, count),
        in_specs=[VMEM_SPEC] + [HBM_SPEC] * count,
        out_specs=[VMEM_SPEC] * count,
        out_shape=[pltpu.VMEM(a.shape, a.dtype) for a in arrays],
        scratch_shapes=[pltpu.SemaphoreType.DMA((4 * count,))],
        compiler_params=pltpu.CompilerParams(vmem_limit_bytes=1024 * 1024),
        name="load",
    )(in_vmem(after), *[in_hbm(a) for a in arrays])


def prepare(x, c, chunks, gain_ref, scaled_ref, inverse_ref):
    count = chunks[0].shape[0]
    for half in range(HALVES):
        prepare_half(
            x, c, chunks[5 * half : 5 * half + 5], gain_ref,
            scaled_ref.at[half * count : (half + 1) * count, :],
            inverse_ref.at[half * count : (half + 1) * count, :],
        )


def prepare_half(x, c, chunks, gain_ref, scaled_ref, inverse_ref):
    def one(step, carry):
        rows = pl.ds(pl.multiple_of(step * 32, 32), 32)
        squares = None
        for shift in range(4):
            base = lax.rem(x + 4 - shift, 4) * 1024
            for ref, core in ((chunks[shift], c), (chunks[4].at[shift], 1 - c)):
                for y in range(2):
                    block = ref[rows, y * 256 : (y + 1) * 256].astype(f32)
                    off = pl.multiple_of(base + y * 512 + core * 256, 256)
                    scaled_ref[rows, pl.ds(off, 256)] = (
                        block * gain_ref[:, pl.ds(off, 256)]
                    ).astype(bf16)
                    part = block[:, :128] * block[:, :128] + block[:, 128:] * block[:, 128:]
                    squares = part if squares is None else squares + part
        total = jnp.sum(squares, axis=1, keepdims=True)
        inverse_ref[rows, :] = jnp.broadcast_to(lax.rsqrt(total / 4096 + norm_eps), (32, 128))
        return carry

    lax.fori_loop(0, chunks[0].shape[0] // 32, one, 0)


def activated(gate, up, inverse):
    gate = gate * inverse
    return gate / (1.0 + jnp.exp(-gate)) * (up * inverse)


def hidden_units(scaled, wg, wu, inverse_ref, gate_ref, up_ref, wait):
    def one(k, carry):
        wait(0, k)
        wait(1, k)
        cols = pl.ds(pl.multiple_of(k * 1024, 1024), 1024)
        part = scaled[:, cols]
        gate = jnp.dot(part, wg[0, cols, :], preferred_element_type=f32)
        up = jnp.dot(part, wu[0, cols, :], preferred_element_type=f32)
        gate_ref[...] = jnp.where(k == 0, gate, gate_ref[...] + gate)
        up_ref[...] = jnp.where(k == 0, up, up_ref[...] + up)
        return carry

    lax.fori_loop(0, 4, one, 0)
    return activated(gate_ref[...], up_ref[...], inverse_ref[:, :1])


def mean_tokens(value):
    rows, cols = value.shape
    return jnp.sum(value.reshape(rows // 32, 32, cols), axis=1) * (1.0 / 32)


def base_means(chunks):
    return jnp.concatenate(
        [mean_tokens(chunks[5 * half][...].astype(f32)) for half in range(HALVES)], axis=0
    )


def mlp_kernel(pool, place, *refs):
    count = 5 * HALVES
    chunks, (gain, wg, wu, wd) = refs[:count], refs[count : count + 4]
    outs = refs[count + 4 : -2]
    send, keep = outs[:HALVES], outs[HALVES : 2 * HALVES]
    scaled, inverse = refs[-2:]
    x, c = place[0], place[1]
    prepare(x, c, chunks, gain, scaled, inverse)
    gate = jnp.dot(scaled[...], wg[0], preferred_element_type=f32)
    up = jnp.dot(scaled[...], wu[0], preferred_element_type=f32)
    hidden = activated(gate, up, inverse[:, :1])
    if pool:
        outs[-2][...] = mean_tokens(hidden)
        outs[-1][...] = base_means(chunks)
    rounded = hidden.astype(bf16)
    first = c == 0
    rows_half = chunks[0].shape[0]

    def one(s, carry):
        rows = pl.multiple_of(lax.rem(x + s, 4) * 1024, 1024)
        term = nt_dot(rounded, wd[0, pl.ds(rows, 1024), :])
        for y in range(2):
            a = term[:, y * 512 : y * 512 + 256]
            b = term[:, y * 512 + 256 : y * 512 + 512]
            cols = slice(y * 256, (y + 1) * 256)
            mine = jnp.where(first, a, b).astype(bf16)
            other = jnp.where(first, b, a).astype(bf16)
            for half in range(HALVES):
                part = slice(half * rows_half, (half + 1) * rows_half)
                keep[half][s, :, cols] = mine[part]
                send[half][s, :, cols] = other[part]
        return carry

    lax.fori_loop(0, 4, one, 0)


def last_kernel(count, place, *refs):
    first = 5 * HALVES
    chunks, gain, before = refs[:first], refs[first], refs[first + 1 : first + 1 + count]
    far, (out, base) = refs[first + 1 + count : first + 4 + count], refs[-10:-8]
    held, sems = refs[-8:-5], refs[-5]
    scaled, inverse, gate, up = refs[-4:]

    def copy(kind, k):
        rows = pl.ds(pl.multiple_of(k * 1024, 1024), 1024)
        return pltpu.make_async_copy(
            far[kind].at[0, rows, :], held[kind].at[0, rows, :], sems.at[kind * 4 + k]
        )

    def begin(k, carry):
        copy(0, k).start()
        copy(1, k).start()
        return carry

    def begin_down(k, carry):
        copy(2, k).start()
        return carry

    lax.fori_loop(0, 4, begin, 0)
    lax.fori_loop(0, 4, begin_down, 0)
    prepare(place[0], place[1], chunks, gain, scaled, inverse)
    hidden = hidden_units(
        scaled, held[0], held[1], inverse, gate, up, lambda kind, k: copy(kind, k).wait()
    )
    base[...] = base_means(chunks)
    every = jnp.concatenate([ref[...] for ref in before] + [mean_tokens(hidden)], axis=0)
    high = every.astype(bf16)
    low = (every - high.astype(f32)).astype(bf16)
    rows = every.shape[0]
    stacked = jnp.concatenate([high, low], axis=0)

    def one(k, carry):
        copy(2, k).wait()
        term = nt_dot(stacked, held[2][0, pl.ds(pl.multiple_of(k * 1024, 1024), 1024), :])
        term = term[:rows] + term[rows:]
        for m in range(4):
            out[4 * k + m] = term[:, m * 256 : (m + 1) * 256]
        return carry

    lax.fori_loop(0, 4, one, 0)


def gathered_kernel(own, a, b, d, out):
    out[...] = (
        own[...].astype(f32) + a[...].astype(f32) + (b[...].astype(f32) + d[...].astype(f32))
    ).astype(bf16)


def by_y(flag, own, peer):
    first = flag[2] == 0
    low, high = own[...].astype(f32), peer[...].astype(f32)
    return jnp.concatenate(
        [jnp.where(first, low, high), jnp.where(first, high, low)], axis=1
    )


def fresh_kernel(flag, own, peer, *out):
    whole = by_y(flag, own, peer).astype(bf16)
    rows = out[0].shape[0]
    for i, ref in enumerate(out):
        ref[...] = whole[i * rows : (i + 1) * rows]


def halves_kernel(keep, got, own, right, across, left):
    own[...] = keep[0].astype(f32) + got[0].astype(f32)
    right[...] = (keep[1].astype(f32) + got[1].astype(f32)).astype(bf16)
    across[...] = (keep[2].astype(f32) + got[2].astype(f32)).astype(bf16)
    left[...] = keep[3].astype(f32) + got[3].astype(f32)


def stack_kernel(a, b, d, e, out):
    for i, ref in enumerate((a, b, d, e)):
        out[i] = ref[...]


def relay_kernel(left, passing, out):
    out[...] = (left[...] + passing[...].astype(f32)).astype(bf16)


def total_kernel(flag, own, state, a, b, out):
    base = jnp.where(flag[2] == 0, state[...].astype(f32), 0.0)
    out[...] = (own[...] + base + (a[...].astype(f32) + b[...].astype(f32))).astype(bf16)


def join_kernel(flag, a, b, out):
    out[...] = (a[...].astype(f32) + b[...].astype(f32)).astype(bf16)


def join_fresh_kernel(flag, a, b, fresh, out):
    joined = (a[...].astype(f32) + b[...].astype(f32)).astype(bf16)
    out[...] = jnp.where(flag[3] == 0, fresh[...], joined)


def local(kernel, scalars, values, outs, scratch=(), limit=4, far=()):
    single = not isinstance(outs, list)
    return pl.pallas_call(
        kernel,
        in_specs=[SMEM_SPEC] * len(scalars) + [VMEM_SPEC] * len(values) + [HBM_SPEC] * len(far),
        out_specs=VMEM_SPEC if single else [VMEM_SPEC] * len(outs),
        out_shape=outs,
        scratch_shapes=list(scratch),
        compiler_params=pltpu.CompilerParams(vmem_limit_bytes=limit * 1024 * 1024),
    )(*scalars, *[in_vmem(v) for v in values], *[in_hbm(v) for v in far])


def out_vmem(shape, dtype):
    return pltpu.VMEM(shape, dtype)


def mlp_scratch(tokens):
    return [
        pltpu.VMEM((tokens, 4096), bf16),
        pltpu.VMEM((tokens, 128), f32),
        pltpu.VMEM((tokens, 640), f32),
        pltpu.VMEM((tokens, 640), f32),
    ]


def call_mlp(place, chunks, gain, weights, pool):
    count = chunks[0].shape[0]
    tokens = count * HALVES
    outs = [out_vmem((4, count, 512), bf16)] * (2 * HALVES)
    if pool:
        outs += [out_vmem((tokens // 32, 640), f32), out_vmem((tokens // 32, 512), f32)]
    result = local(
        functools.partial(mlp_kernel, pool), [place], [*chunks, gain, *weights], outs,
        mlp_scratch(tokens)[:2], 16,
    )
    return result[:HALVES], result[HALVES : 2 * HALVES], result[2 * HALVES :]


def call_last(place, chunks, gain, far, before):
    tokens = chunks[0].shape[0] * HALVES
    rows = sum(b.shape[0] for b in before) + tokens // 32
    return local(
        functools.partial(last_kernel, len(before)), [place], [*chunks, gain, *before],
        [out_vmem((16, rows, 256), f32), out_vmem((tokens // 32, 512), f32)],
        [pltpu.VMEM((1, 4096, 640), bf16)] * 3
        + [pltpu.SemaphoreType.DMA((12,))]
        + mlp_scratch(tokens),
        28, far,
    )


def head_kernel(place, chosen_ref, all_ref, gain_ref, head_ref, out_ref):
    total = squares = None
    for m in range(16):
        cols = slice(m * 256, (m + 1) * 256)
        side = (m // 2) % 2
        v = jnp.concatenate([all_ref[side, m], all_ref[1 - side, m]], axis=0)
        now = jnp.dot(v, head_ref[cols, :], preferred_element_type=f32)
        total = now if total is None else total + now
        plain = v.astype(f32) / gain_ref[:, cols]
        plain = plain * plain
        plain = plain[:, :128] + plain[:, 128:]
        squares = plain if squares is None else squares + plain
    factor = lax.rsqrt(jnp.sum(squares, axis=1, keepdims=True) / 4096 + final_eps)
    here = place[0]
    side = lax.rem(here // 2, 2)
    mine = jnp.concatenate([all_ref[side, here], all_ref[1 - side, here]], axis=0)
    mine = mine.astype(f32) * factor
    scores = lax.dot_general(
        total * factor, mine, (((1,), (1,)), ((), ())),
        precision=lax.Precision.HIGHEST, preferred_element_type=f32,
    )
    skew = scores - scores.T
    chosen = chosen_ref[...]
    count = skew.shape[0]
    hot = (lax.broadcasted_iota(jnp.int32, (chosen.shape[0], count), 1) == chosen).astype(f32)
    half = out_ref.shape[0]
    rows = jnp.dot(hot[: 2 * half], skew, precision=lax.Precision.HIGHEST, preferred_element_type=f32)
    tile = lax.dot_general(
        rows, hot, (((1,), (1,)), ((), ())),
        precision=lax.Precision.HIGHEST, preferred_element_type=f32,
    )
    lane = lax.broadcasted_iota(jnp.int32, out_ref.shape, 1)
    out_ref[...] = jnp.where(lane < half, tile[:half], tile[half:])


def head_part(place, chosen, everyone, gain, head):
    vmem = pl.BlockSpec(memory_space=pltpu.VMEM)
    return pl.pallas_call(
        head_kernel,
        in_specs=[pl.BlockSpec(memory_space=pltpu.SMEM)] + [vmem] * 4,
        out_specs=vmem,
        out_shape=jax.ShapeDtypeStruct((GROUP, chosen.shape[0]), f32),
        name="head",
    )(place, chosen, everyone, gain, head)


def per_device(
    token_ids, members, owners, embed_table, norm_gain, gate_weight, up_weight, down_weight,
    final_gain, head_weight,
):
    section = lax.axis_index("section")
    mp = lax.axis_index("mp")
    dp = lax.axis_index("dp")
    x, y, c = mp // 4, (mp // 2) % 2, mp % 2
    place = jnp.stack([x, c, y, section]).astype(jnp.int32)
    ids = jnp.where(y == 0, token_ids, other_dp(token_ids))
    flat = ids.reshape(1, -1) - section * embed_table.shape[1]
    together = flat.shape[1] // BLOCKS
    size = (together // HALVES, 512)

    def summed(part):
        pieces = []
        for z in (1, 3, 2):
            pieces.append(along_sections(part, z))
        return local(gathered_kernel, [], [part, *pieces], out_vmem(part.shape, bf16), ())

    def start_of(own):
        return local(
            fresh_kernel, [place], [own, other_y(own)], [out_vmem(size, bf16)] * HALVES, ()
        )

    part = embed_part(place, flat, 0, together, embed_table)
    own = summed(part)
    weights = loaded(part, gate_weight, up_weight, down_weight)
    states = start_of(own)
    sums_state, sums_hidden = [], []
    ticks = BLOCKS + 3
    for tick in range(ticks):
        chunks = []
        for state in states:
            near = along_x(state, 1)
            mine = [state, near, along_x(near, 1), along_x(state, 3)]
            stacked = local(stack_kernel, [], mine, out_vmem((4, *size), bf16), ())
            chunks += [*mine, other_core(stacked)]
        if tick == ticks - 1:
            far = (gate_weight, up_weight, down_weight)
            terms, base = call_last(place, chunks, norm_gain, far, sums_hidden)
            sums_state.append(base)
            break
        send, keep, pooled = call_mlp(place, chunks, norm_gain, weights, tick >= 3)
        if tick >= 3:
            sums_hidden.append(pooled[0])
            sums_state.append(pooled[1])
        moving = []
        for half in range(HALVES):
            own, right, across, left = local(
                halves_kernel, [], [keep[half], other_core(send[half])],
                [out_vmem(size, t) for t in (f32, bf16, bf16, f32)], (),
            )
            passing = along_x(across, 3)
            arrived = [along_x(right, 1)]
            left = local(relay_kernel, [], [left, passing], out_vmem(size, bf16), ())
            arrived.append(along_x(left, 3))
            moving.append((own, arrived))
        if tick + 1 < BLOCKS:
            part = embed_part(place, flat, (tick + 1) * together, together, embed_table)
        if tick + 1 < BLOCKS:
            fresh = start_of(summed(part))
        following = []
        for half, (own, arrived) in enumerate(moving):
            total = local(
                total_kernel, [place], [own, states[half], *arrived], out_vmem(size, bf16), (),
            )
            ahead, kernel = [onward(total, 0), onward(total, 1)], join_kernel
            if tick + 1 < BLOCKS:
                ahead, kernel = [*ahead, fresh[half]], join_fresh_kernel
            following.append(local(kernel, [place], ahead, out_vmem(size, bf16), ()))
        states = following
    owners, members, final_gain, terms = lax.optimization_barrier(
        (owners, members, final_gain, terms)
    )

    groups = [[(g ^ ((m // 2) % 2)) * 16 + m for m in range(16)] for g in range(2)]
    pieces = lax.all_to_all(
        terms, ("dp", "mp"), 0, 0, tiled=True, axis_index_groups=groups
    )
    base = jnp.concatenate(sums_state, axis=0)
    pooled = jnp.sum(pieces, axis=0) + jnp.where(y == 0, base[:, :256], base[:, 256:])
    gain_here = lax.dynamic_slice_in_dim(final_gain, mp * 256, 256)
    value = (pooled * gain_here[None, :]).astype(bf16)
    everyone = lax.all_to_all(
        jnp.broadcast_to(value, (32, *value.shape)), ("dp", "mp"), 0, 0, tiled=True
    ).reshape(2, 16, *value.shape)

    prompts = owners.shape[0]
    here = prompts // 2
    slots = dp * here + jnp.arange(here, dtype=jnp.int32)
    match = (owners[None, :] == slots[:, None]).astype(jnp.int32)
    hit = match[:, :, None] * members.reshape(prompts, GROUP)[None]
    chosen = jnp.sum(hit, axis=1).reshape(here * GROUP, 1)
    chosen = jnp.pad(chosen, ((0, 128 - here * GROUP), (0, 0)), constant_values=-1)
    tile = head_part(
        jnp.reshape(mp, (1,)).astype(jnp.int32), chosen, everyone, final_gain[None], head_weight
    )
    rows = GROUP // 4
    got = lax.all_to_all(
        jnp.broadcast_to(tile, (16, GROUP, 128)), "mp", 0, 0, tiled=True
    )
    skew = jnp.sum(got, axis=0)
    options = jnp.stack([along_sections(skew, (s + 1) % 4) for s in range(3)] + [skew])
    skew = lax.dynamic_index_in_dim(options, section, 0, keepdims=False)
    skew = lax.dynamic_slice_in_dim(skew, section * rows, rows, 0)
    skew = jnp.stack([skew[:, p * GROUP : (p + 1) * GROUP] for p in range(here)])
    return jax.nn.sigmoid(skew)


def solution(mesh):
    placed = (
        P("dp", None),
        P(),
        P(),
        P("mp", "section"),
        P("section", None),
        P("section", None, "mp"),
        P("section", None, "mp"),
        P("section", None, "mp"),
        P(),
        P(None, "mp"),
    )
    return jax.shard_map(
        per_device, mesh=mesh, in_specs=placed, out_specs=P("dp", "section", None),
        check_vma=False,
    )
```

```python
import functools

import jax
import jax.numpy as jnp
from jax import lax
from jax.experimental import pallas as pl
from jax.experimental.pallas import tpu as pltpu
from jax.sharding import PartitionSpec as P


GROUP = 8
BLOCKS = 2
HALVES = 2
AXES = ("dp", "section", "mp")

norm_eps = 1e-05
final_eps = 1e-06
bf16 = jnp.bfloat16
f32 = jnp.float32


def moved(value, target):
    pairs = []
    for dp in range(2):
        for z in range(4):
            for x in range(4):
                for y in range(2):
                    for c in range(2):
                        to = target(dp, z, x, y, c)
                        if to is not None:
                            d, s, a, b, e = to
                            pairs.append(
                                (dp * 64 + z * 16 + x * 4 + y * 2 + c, d * 64 + s * 16 + a * 4 + b * 2 + e)
                            )
    return lax.ppermute(value, AXES, pairs)


def along_x(value, shift):
    return moved(value, lambda d, z, x, y, c: (d, z, (x + shift) % 4, y, c))


def other_core(value):
    return moved(value, lambda d, z, x, y, c: (d, z, x, y, 1 - c))


def other_dp(value):
    return moved(value, lambda d, z, x, y, c: (1 - d, z, x, y, c))


def other_y(value):
    return moved(value, lambda d, z, x, y, c: (1 - d, z, x, 1 - y, c))


def along_sections(value, shift):
    return moved(value, lambda d, z, x, y, c: (d, (z + shift) % 4, x, y, c))


def onward(value, flip):
    return moved(value, lambda d, z, x, y, c: (d ^ flip, (z + 1) % 4, x, y ^ flip, c))


def nt_dot(a, b):
    return lax.dot_general(a, b, (((1,), (1,)), ((), ())), preferred_element_type=f32)


def embed_kernel(width, first, place, ids_ref, table_ref, out, held, sems):
    rows = out.shape[0]
    ids = ids_ref[:, first : first + rows]
    steps = table_ref.shape[1] // width

    def copy(step):
        cols = pl.ds(pl.multiple_of(step * width, width), width)
        return pltpu.make_async_copy(table_ref.at[:, cols], held.at[:, cols], sems.at[step])

    def begin(step, carry):
        copy(step).start()
        return carry

    lax.fori_loop(0, steps, begin, 0)

    def one(step, acc):
        copy(step).wait()
        start = pl.multiple_of(step * width, width)
        hot = lax.broadcasted_iota(jnp.int32, (width, rows), 0) == ids - start
        return acc + jnp.dot(
            held[:, pl.ds(start, width)], hot.astype(f32).astype(bf16), preferred_element_type=f32
        )

    acc = lax.fori_loop(0, steps, one, jnp.zeros((table_ref.shape[0], rows), f32))
    out[...] = acc.T.astype(bf16)


def cost(products):
    return pl.CostEstimate(flops=2 * products, bytes_accessed=0, transcendentals=0)


def in_hbm(value):
    return pltpu.with_memory_space_constraint(value, pltpu.HBM)


def in_vmem(value):
    return pltpu.with_memory_space_constraint(value, pltpu.VMEM)


VMEM_SPEC = pl.BlockSpec(memory_space=pltpu.VMEM)
HBM_SPEC = pl.BlockSpec(memory_space=pltpu.HBM)
SMEM_SPEC = pl.BlockSpec(memory_space=pltpu.SMEM)


def embed_part(place, ids, first, rows, table):
    width = 2048
    return pl.pallas_call(
        functools.partial(embed_kernel, width, first),
        in_specs=[SMEM_SPEC, VMEM_SPEC, HBM_SPEC],
        out_specs=VMEM_SPEC,
        out_shape=pltpu.VMEM((rows, table.shape[0]), bf16),
        scratch_shapes=[
            pltpu.VMEM(table.shape, bf16),
            pltpu.SemaphoreType.DMA((table.shape[1] // width,)),
        ],
        compiler_params=pltpu.CompilerParams(vmem_limit_bytes=20 * 1024 * 1024),
        cost_estimate=cost(rows * table.size),
        name="embed",
    )(place, in_vmem(ids), in_hbm(table))


def load_kernel(count, after, *refs):
    sources, places, sems = refs[:count], refs[count : 2 * count], refs[-1]
    copies = []
    for i, (source, place) in enumerate(zip(sources, places)):
        rows = source.shape[1] // 4
        for k in range(4):
            where = (0, pl.ds(k * rows, rows))
            copies.append(
                pltpu.make_async_copy(source.at[where], place.at[where], sems.at[4 * i + k])
            )
    for copy in copies:
        copy.start()
    for copy in copies:
        copy.wait()


def loaded(after, *arrays):
    count = len(arrays)
    return pl.pallas_call(
        functools.partial(load_kernel, count),
        in_specs=[VMEM_SPEC] + [HBM_SPEC] * count,
        out_specs=[VMEM_SPEC] * count,
        out_shape=[pltpu.VMEM(a.shape, a.dtype) for a in arrays],
        scratch_shapes=[pltpu.SemaphoreType.DMA((4 * count,))],
        compiler_params=pltpu.CompilerParams(vmem_limit_bytes=1024 * 1024),
        name="load",
    )(in_vmem(after), *[in_hbm(a) for a in arrays])


def prepare(x, c, chunks, gain_ref, scaled_ref, inverse_ref):
    count = chunks[0].shape[0]
    for half in range(HALVES):
        prepare_half(
            x, c, chunks[8 * half : 8 * half + 8], gain_ref,
            scaled_ref.at[half * count : (half + 1) * count, :],
            inverse_ref.at[half * count : (half + 1) * count, :],
        )


def prepare_half(x, c, chunks, gain_ref, scaled_ref, inverse_ref):
    def one(step, carry):
        rows = pl.ds(pl.multiple_of(step * 32, 32), 32)
        squares = None
        for shift in range(4):
            base = lax.rem(x + 4 - shift, 4) * 1024
            for ref, core in ((chunks[shift], c), (chunks[4 + shift], 1 - c)):
                for y in range(2):
                    block = ref[rows, y * 256 : (y + 1) * 256].astype(f32)
                    off = pl.multiple_of(base + y * 512 + core * 256, 256)
                    scaled_ref[rows, pl.ds(off, 256)] = (
                        block * gain_ref[:, pl.ds(off, 256)]
                    ).astype(bf16)
                    part = block[:, :128] * block[:, :128] + block[:, 128:] * block[:, 128:]
                    squares = part if squares is None else squares + part
        total = jnp.sum(squares, axis=1, keepdims=True)
        inverse_ref[rows, :] = jnp.broadcast_to(lax.rsqrt(total / 4096 + norm_eps), (32, 128))
        return carry

    lax.fori_loop(0, chunks[0].shape[0] // 32, one, 0)


def activated(gate, up, inverse):
    gate = gate * inverse
    return gate / (1.0 + jnp.exp(-gate)) * (up * inverse)


def hidden_units(scaled, wg, wu, inverse_ref, gate_ref, up_ref, wait):
    def one(k, carry):
        wait(0, k)
        wait(1, k)
        cols = pl.ds(pl.multiple_of(k * 1024, 1024), 1024)
        part = scaled[:, cols]
        gate = jnp.dot(part, wg[0, cols, :], preferred_element_type=f32)
        up = jnp.dot(part, wu[0, cols, :], preferred_element_type=f32)
        gate_ref[...] = jnp.where(k == 0, gate, gate_ref[...] + gate)
        up_ref[...] = jnp.where(k == 0, up, up_ref[...] + up)
        return carry

    lax.fori_loop(0, 4, one, 0)
    return activated(gate_ref[...], up_ref[...], inverse_ref[:, :1])


def mean_tokens(value):
    rows, cols = value.shape
    return jnp.sum(value.reshape(rows // 32, 32, cols), axis=1) * (1.0 / 32)


def base_means(chunks):
    return jnp.concatenate(
        [mean_tokens(chunks[8 * half][...].astype(f32)) for half in range(HALVES)], axis=0
    )


def mlp_kernel(pool, place, *refs):
    count = 8 * HALVES
    chunks, (gain, wg, wu, wd) = refs[:count], refs[count : count + 4]
    outs = refs[count + 4 : -2]
    send, keep = outs[:HALVES], outs[HALVES : 2 * HALVES]
    scaled, inverse = refs[-2:]
    x, c = place[0], place[1]
    prepare(x, c, chunks, gain, scaled, inverse)
    gate = jnp.dot(scaled[...], wg[0], preferred_element_type=f32)
    up = jnp.dot(scaled[...], wu[0], preferred_element_type=f32)
    hidden = activated(gate, up, inverse[:, :1])
    if pool:
        outs[-2][...] = mean_tokens(hidden)
        outs[-1][...] = base_means(chunks)
    rounded = hidden.astype(bf16)
    first = c == 0
    rows_half = chunks[0].shape[0]

    def one(s, carry):
        rows = pl.multiple_of(lax.rem(x + s, 4) * 1024, 1024)
        term = nt_dot(rounded, wd[0, pl.ds(rows, 1024), :])
        for y in range(2):
            a = term[:, y * 512 : y * 512 + 256]
            b = term[:, y * 512 + 256 : y * 512 + 512]
            cols = slice(y * 256, (y + 1) * 256)
            mine = jnp.where(first, a, b).astype(bf16)
            other = jnp.where(first, b, a).astype(bf16)
            for half in range(HALVES):
                part = slice(half * rows_half, (half + 1) * rows_half)
                keep[half][s, :, cols] = mine[part]
                send[half][s, :, cols] = other[part]
        return carry

    lax.fori_loop(0, 4, one, 0)


def last_kernel(count, place, *refs):
    first = 8 * HALVES
    chunks, gain, before = refs[:first], refs[first], refs[first + 1 : first + 1 + count]
    far, (out, base) = refs[first + 1 + count : first + 4 + count], refs[-10:-8]
    held, sems = refs[-8:-5], refs[-5]
    scaled, inverse, gate, up = refs[-4:]

    def copy(kind, k):
        rows = pl.ds(pl.multiple_of(k * 1024, 1024), 1024)
        return pltpu.make_async_copy(
            far[kind].at[0, rows, :], held[kind].at[0, rows, :], sems.at[kind * 4 + k]
        )

    def begin(k, carry):
        copy(0, k).start()
        copy(1, k).start()
        return carry

    def begin_down(k, carry):
        copy(2, k).start()
        return carry

    lax.fori_loop(0, 4, begin, 0)
    lax.fori_loop(0, 4, begin_down, 0)
    prepare(place[0], place[1], chunks, gain, scaled, inverse)
    hidden = hidden_units(
        scaled, held[0], held[1], inverse, gate, up, lambda kind, k: copy(kind, k).wait()
    )
    base[...] = base_means(chunks)
    every = jnp.concatenate([ref[...] for ref in before] + [mean_tokens(hidden)], axis=0)
    high = every.astype(bf16)
    low = (every - high.astype(f32)).astype(bf16)
    rows = every.shape[0]
    stacked = jnp.concatenate([high, low], axis=0)

    def one(k, carry):
        copy(2, k).wait()
        term = nt_dot(stacked, held[2][0, pl.ds(pl.multiple_of(k * 1024, 1024), 1024), :])
        term = term[:rows] + term[rows:]
        for m in range(4):
            out[4 * k + m] = term[:, m * 256 : (m + 1) * 256]
        return carry

    lax.fori_loop(0, 4, one, 0)


def gathered_kernel(own, a, b, d, out):
    out[...] = (
        own[...].astype(f32) + a[...].astype(f32) + (b[...].astype(f32) + d[...].astype(f32))
    ).astype(bf16)


def by_y(flag, own, peer):
    first = flag[2] == 0
    low, high = own[...].astype(f32), peer[...].astype(f32)
    return jnp.concatenate(
        [jnp.where(first, low, high), jnp.where(first, high, low)], axis=1
    )


def fresh_kernel(flag, own, peer, *out):
    whole = by_y(flag, own, peer).astype(bf16)
    rows = out[0].shape[0]
    for i, ref in enumerate(out):
        ref[...] = whole[i * rows : (i + 1) * rows]


def halves_kernel(keep, got, own, *out):
    own[...] = keep[0].astype(f32) + got[0].astype(f32)
    for s in range(1, 4):
        out[s - 1][...] = (keep[s].astype(f32) + got[s].astype(f32)).astype(bf16)


def total_kernel(flag, own, state, a, b, d, out):
    base = jnp.where(flag[2] == 0, state[...].astype(f32), 0.0)
    out[...] = (
        own[...] + base + (a[...].astype(f32) + b[...].astype(f32) + d[...].astype(f32))
    ).astype(bf16)


def join_kernel(flag, a, b, out):
    out[...] = (a[...].astype(f32) + b[...].astype(f32)).astype(bf16)


def join_fresh_kernel(flag, a, b, fresh, out):
    joined = (a[...].astype(f32) + b[...].astype(f32)).astype(bf16)
    out[...] = jnp.where(flag[3] == 0, fresh[...], joined)


def local(kernel, scalars, values, outs, scratch=(), limit=4, far=()):
    single = not isinstance(outs, list)
    return pl.pallas_call(
        kernel,
        in_specs=[SMEM_SPEC] * len(scalars) + [VMEM_SPEC] * len(values) + [HBM_SPEC] * len(far),
        out_specs=VMEM_SPEC if single else [VMEM_SPEC] * len(outs),
        out_shape=outs,
        scratch_shapes=list(scratch),
        compiler_params=pltpu.CompilerParams(vmem_limit_bytes=limit * 1024 * 1024),
    )(*scalars, *[in_vmem(v) for v in values], *[in_hbm(v) for v in far])


def out_vmem(shape, dtype):
    return pltpu.VMEM(shape, dtype)


def mlp_scratch(tokens):
    return [
        pltpu.VMEM((tokens, 4096), bf16),
        pltpu.VMEM((tokens, 128), f32),
        pltpu.VMEM((tokens, 640), f32),
        pltpu.VMEM((tokens, 640), f32),
    ]


def call_mlp(place, chunks, gain, weights, pool):
    count = chunks[0].shape[0]
    tokens = count * HALVES
    outs = [out_vmem((4, count, 512), bf16)] * (2 * HALVES)
    if pool:
        outs += [out_vmem((tokens // 32, 640), f32), out_vmem((tokens // 32, 512), f32)]
    result = local(
        functools.partial(mlp_kernel, pool), [place], [*chunks, gain, *weights], outs,
        mlp_scratch(tokens)[:2], 16,
    )
    return result[:HALVES], result[HALVES : 2 * HALVES], result[2 * HALVES :]


def call_last(place, chunks, gain, far, before):
    tokens = chunks[0].shape[0] * HALVES
    rows = sum(b.shape[0] for b in before) + tokens // 32
    return local(
        functools.partial(last_kernel, len(before)), [place], [*chunks, gain, *before],
        [out_vmem((16, rows, 256), f32), out_vmem((tokens // 32, 512), f32)],
        [pltpu.VMEM((1, 4096, 640), bf16)] * 3
        + [pltpu.SemaphoreType.DMA((12,))]
        + mlp_scratch(tokens),
        28, far,
    )


def head_kernel(place, chosen_ref, all_ref, gain_ref, head_ref, out_ref):
    total = squares = None
    for m in range(16):
        cols = slice(m * 256, (m + 1) * 256)
        side = (m // 2) % 2
        v = jnp.concatenate([all_ref[side, m], all_ref[1 - side, m]], axis=0)
        now = jnp.dot(v, head_ref[cols, :], preferred_element_type=f32)
        total = now if total is None else total + now
        plain = v.astype(f32) / gain_ref[:, cols]
        plain = plain * plain
        plain = plain[:, :128] + plain[:, 128:]
        squares = plain if squares is None else squares + plain
    factor = lax.rsqrt(jnp.sum(squares, axis=1, keepdims=True) / 4096 + final_eps)
    here = place[0]
    side = lax.rem(here // 2, 2)
    mine = jnp.concatenate([all_ref[side, here], all_ref[1 - side, here]], axis=0)
    mine = mine.astype(f32) * factor
    scores = lax.dot_general(
        total * factor, mine, (((1,), (1,)), ((), ())),
        precision=lax.Precision.HIGHEST, preferred_element_type=f32,
    )
    skew = scores - scores.T
    chosen = chosen_ref[...]
    count = skew.shape[0]
    hot = (lax.broadcasted_iota(jnp.int32, (chosen.shape[0], count), 1) == chosen).astype(f32)
    half = out_ref.shape[0]
    rows = jnp.dot(hot[: 2 * half], skew, precision=lax.Precision.HIGHEST, preferred_element_type=f32)
    tile = lax.dot_general(
        rows, hot, (((1,), (1,)), ((), ())),
        precision=lax.Precision.HIGHEST, preferred_element_type=f32,
    )
    lane = lax.broadcasted_iota(jnp.int32, out_ref.shape, 1)
    out_ref[...] = jnp.where(lane < half, tile[:half], tile[half:])


def head_part(place, chosen, everyone, gain, head):
    vmem = pl.BlockSpec(memory_space=pltpu.VMEM)
    return pl.pallas_call(
        head_kernel,
        in_specs=[pl.BlockSpec(memory_space=pltpu.SMEM)] + [vmem] * 4,
        out_specs=vmem,
        out_shape=jax.ShapeDtypeStruct((GROUP, chosen.shape[0]), f32),
        name="head",
    )(place, chosen, everyone, gain, head)


def per_device(
    token_ids, members, owners, embed_table, norm_gain, gate_weight, up_weight, down_weight,
    final_gain, head_weight,
):
    section = lax.axis_index("section")
    mp = lax.axis_index("mp")
    dp = lax.axis_index("dp")
    x, y, c = mp // 4, (mp // 2) % 2, mp % 2
    place = jnp.stack([x, c, y, section]).astype(jnp.int32)
    ids = jnp.where(y == 0, token_ids, other_dp(token_ids))
    flat = ids.reshape(1, -1) - section * embed_table.shape[1]
    together = flat.shape[1] // BLOCKS
    size = (together // HALVES, 512)

    def summed(part):
        pieces = []
        for z in (1, 3, 2):
            pieces.append(along_sections(part, z))
        return local(gathered_kernel, [], [part, *pieces], out_vmem(part.shape, bf16), ())

    def start_of(own):
        return local(
            fresh_kernel, [place], [own, other_y(own)], [out_vmem(size, bf16)] * HALVES, ()
        )

    part = embed_part(place, flat, 0, together, embed_table)
    own = summed(part)
    weights = loaded(part, gate_weight, up_weight, down_weight)
    states = start_of(own)
    sums_state, sums_hidden = [], []
    ticks = BLOCKS + 3
    for tick in range(ticks):
        chunks = []
        for state in states:
            near = along_x(state, 1)
            mine = [state, near, along_x(near, 1), along_x(state, 3)]
            chunks += [*mine, *[other_core(m) for m in mine]]
        if tick == ticks - 1:
            far = (gate_weight, up_weight, down_weight)
            terms, base = call_last(place, chunks, norm_gain, far, sums_hidden)
            sums_state.append(base)
            break
        send, keep, pooled = call_mlp(place, chunks, norm_gain, weights, tick >= 3)
        if tick >= 3:
            sums_hidden.append(pooled[0])
            sums_state.append(pooled[1])
        moving = []
        for half in range(HALVES):
            own, *out = local(
                halves_kernel, [], [keep[half], other_core(send[half])],
                [out_vmem(size, f32)] + [out_vmem(size, bf16)] * 3, (),
            )
            arrived = []
            for s in (1, 2, 3):
                arrived.append(along_x(out[s - 1], s))
            moving.append((own, arrived))
        if tick + 1 < BLOCKS:
            part = embed_part(place, flat, (tick + 1) * together, together, embed_table)
        if tick + 1 < BLOCKS:
            fresh = start_of(summed(part))
        following = []
        for half, (own, arrived) in enumerate(moving):
            total = local(
                total_kernel, [place], [own, states[half], *arrived], out_vmem(size, bf16), (),
            )
            ahead, kernel = [onward(total, 0), onward(total, 1)], join_kernel
            if tick + 1 < BLOCKS:
                ahead, kernel = [*ahead, fresh[half]], join_fresh_kernel
            following.append(local(kernel, [place], ahead, out_vmem(size, bf16), ()))
        states = following
    owners, members, final_gain, terms = lax.optimization_barrier(
        (owners, members, final_gain, terms)
    )

    groups = [[(g ^ ((m // 2) % 2)) * 16 + m for m in range(16)] for g in range(2)]
    pieces = lax.all_to_all(
        terms, ("dp", "mp"), 0, 0, tiled=True, axis_index_groups=groups
    )
    base = jnp.concatenate(sums_state, axis=0)
    pooled = jnp.sum(pieces, axis=0) + jnp.where(y == 0, base[:, :256], base[:, 256:])
    gain_here = lax.dynamic_slice_in_dim(final_gain, mp * 256, 256)
    value = (pooled * gain_here[None, :]).astype(bf16)
    everyone = lax.all_to_all(
        jnp.broadcast_to(value, (32, *value.shape)), ("dp", "mp"), 0, 0, tiled=True
    ).reshape(2, 16, *value.shape)

    prompts = owners.shape[0]
    here = prompts // 2
    slots = dp * here + jnp.arange(here, dtype=jnp.int32)
    match = (owners[None, :] == slots[:, None]).astype(jnp.int32)
    hit = match[:, :, None] * members.reshape(prompts, GROUP)[None]
    chosen = jnp.sum(hit, axis=1).reshape(here * GROUP, 1)
    chosen = jnp.pad(chosen, ((0, 128 - here * GROUP), (0, 0)), constant_values=-1)
    tile = head_part(
        jnp.reshape(mp, (1,)).astype(jnp.int32), chosen, everyone, final_gain[None], head_weight
    )
    rows = GROUP // 4
    got = lax.all_to_all(
        jnp.broadcast_to(tile, (16, GROUP, 128)), "mp", 0, 0, tiled=True
    )
    skew = jnp.sum(got, axis=0)
    options = jnp.stack([along_sections(skew, (s + 1) % 4) for s in range(3)] + [skew])
    skew = lax.dynamic_index_in_dim(options, section, 0, keepdims=False)
    skew = lax.dynamic_slice_in_dim(skew, section * rows, rows, 0)
    skew = jnp.stack([skew[:, p * GROUP : (p + 1) * GROUP] for p in range(here)])
    return jax.nn.sigmoid(skew)


def solution(mesh):
    placed = (
        P("dp", None),
        P(),
        P(),
        P("mp", "section"),
        P("section", None),
        P("section", None, "mp"),
        P("section", None, "mp"),
        P("section", None, "mp"),
        P(),
        P(None, "mp"),
    )
    return jax.shard_map(
        per_device, mesh=mesh, in_specs=placed, out_specs=P("dp", "section", None),
        check_vma=False,
    )
```
